32 devices in a mesh: rep: 2 (over y), fsdp: 4 (over z), tp: 4 (over x, core).
Axes of the slice: x: 2, y: 2, z: 4, core: 2. Of those that a mesh axis runs over, the one named last changes fastest.
Arguments:
- hidden_states: bfloat16 [512, 4096], P(('rep', 'fsdp')), may hold values from -240 to 240, as said below
- labels: int32 [512], P(('rep', 'fsdp')), may hold values from 0 to 32767
- head_weight: bfloat16 [32768, 4096], P(('fsdp', 'tp')), may hold values from -0.09375 to 0.09375
- hessian: float32 [32768, 4096], P(('fsdp', 'tp'), 'rep'), may hold values from 0.01 to 1
- momentum: float32 [32768, 4096], P(('fsdp', 'tp'), 'rep'), may hold values from -0.03 to 0.03
Outputs:
- new_hessian: float32 [32768, 4096], P(('fsdp', 'tp'), 'rep')
- step: float32 [32768, 4096], P(('fsdp', 'tp'), 'rep')
The draws below stay inside these ranges and needn't reach their ends.
Inputs may be any that keep to these rules, and one draw needn't show every extreme that they name: `hidden_states`: real values, rows of unequal scale.
All inputs are finite; a program needn't handle non-finite values.
Results may differ from the reference program's by a relative error of at most 0.0007.
Values may be sent and summed in bfloat16 or wider, within the bound.
No kernel may reach another device: no remote copies, remote signals or barrier semaphores. Data moves between devices by JAX's collectives and lax.ppermute only.
A program may use at most 192 MiB of HBM per device.

```python
import math
import jax
import jax.numpy as jnp
from jax import lax

D = 4096
VOCAB = 32768
TOKENS = 512


def draw_hidden_states(key, part):
    first_key, second_key = jax.random.split(jax.random.fold_in(key, 11))
    values = jnp.clip(jax.random.normal(first_key, (TOKENS, D), jnp.float32), -6.0, 6.0)
    scales = jnp.exp(jax.random.uniform(second_key, (TOKENS, 1), jnp.float32, 0.0, math.log(10.0)))
    return (3.0 * values * scales).astype(jnp.bfloat16)


def place_ends(drawn, own_key, smallest, largest):
    place = [jax.random.randint(jax.random.fold_in(own_key, axis), (), 0, length) for axis, length in enumerate(drawn.shape)]
    main_axis = drawn.shape.index(max(drawn.shape))
    next_to = place[:main_axis] + [(place[main_axis] + 1) % drawn.shape[main_axis]] + place[main_axis + 1:]
    return drawn.at[tuple(place)].set(smallest).at[tuple(next_to)].set(largest)


def block_levels(rng, extent, cuts, smallest, largest):
    def one(dim, shards_of):
        heights = jax.random.uniform(jax.random.fold_in(jax.random.fold_in(rng, 6), dim), (shards_of,), jnp.float32, smallest / len(cuts), largest / len(cuts))
        return jnp.repeat(jnp.exp(heights), extent[dim] // shards_of).reshape((-1,) + (1,) * (len(extent) - dim - 1))

    gain = one(*cuts[0])
    for cut in cuts[1:]:
        gain = gain * one(*cut)
    return gain


def gaussian(rng, shape, spread, reach, pieces=(), dtype=jnp.bfloat16):
    values = spread * jax.random.normal(rng, shape, jnp.float32)
    if pieces:
        values = values * block_levels(rng, shape, pieces, -0.22, 0.18)
    return jnp.clip(values, -reach, reach).astype(dtype)


def setup_inputs(seed: int = 0) -> dict:
    key_list = jax.random.split(jax.random.key(seed), 6)
    hidden_states = draw_hidden_states(jax.random.fold_in(key_list[5], 71), 0)
    labels = place_ends(jax.random.randint(key_list[1], (TOKENS,), 0, VOCAB), jax.random.fold_in(key_list[1], 1), 0, VOCAB - 1).astype(jnp.int32)
    head_weight = gaussian(key_list[2], (VOCAB, D), D ** -0.5, 0.09375, ((0, 16),))
    hessian = jnp.clip(jnp.exp(math.log(1.0) - 4.6051702 * jax.random.uniform(key_list[3], (VOCAB, D), jnp.float32) ** block_levels(key_list[3], (VOCAB, D), ((0, 16), (1, 2)), -0.2, 0.2)), 0.01, 1.0)
    momentum = gaussian(key_list[4], (VOCAB, D), 0.005, 0.03, ((0, 16), (1, 2)), jnp.float32)
    return {"hidden_states": hidden_states, "labels": labels, "head_weight": head_weight, "hessian": hessian, "momentum": momentum}


decay_rate = 0.99
clip_scale = 0.05


def reference(hidden_states, labels, head_weight, hessian, momentum):
    logits = lax.dot_general(hidden_states, head_weight, (((1,), (1,)), ((), ())), preferred_element_type=jnp.float32)
    row_max = jnp.max(logits, axis=1)
    weights = jnp.exp(logits - row_max[:, None])
    row_total = jnp.sum(weights, axis=1)
    columns = lax.broadcasted_iota(jnp.int32, (1, logits.shape[1]), 1)
    onehot = (labels[:, None] == columns).astype(jnp.float32)
    residue = weights / row_total[:, None] - onehot
    gradient = lax.dot_general(residue, hidden_states.astype(jnp.float32), (((0,), (0,)), ((), ())), precision=lax.Precision.HIGHEST, preferred_element_type=jnp.float32)
    new_hessian = decay_rate * hessian + (1.0 - decay_rate) * gradient * gradient
    step = jnp.clip(momentum / (clip_scale * new_hessian), -1.0, 1.0)
    return new_hessian, step
```

```python
import functools

import jax
import jax.numpy as jnp
from jax import lax
from jax.experimental import pallas as pl
from jax.experimental.pallas import tpu as pltpu
from jax.sharding import PartitionSpec as P

decay_rate = 0.99
clip_scale = 0.05


LANE = 128
VMEM_BYTES = 56 * 1024 * 1024


def local_large(hidden_states, labels, head_weight, hessian, momentum):
    vocab_rows = head_weight.shape[0]
    tokens, targets = (
        lax.all_gather(hidden_states, "fsdp", axis=0, tiled=True),
        lax.all_gather(labels, "fsdp", axis=0, tiled=True),
    )
    logits = lax.dot_general(
        tokens, head_weight, (((1,), (1,)), ((), ())), preferred_element_type=jnp.float32
    )
    local_max = jnp.max(logits, axis=1)
    row_max = lax.pmax(local_max, ("fsdp", "tp"))
    weights = jnp.exp(logits - row_max[:, None])
    row_total = lax.psum(jnp.sum(weights, axis=1), ("fsdp", "tp"))
    offset = lax.axis_index(("fsdp", "tp")) * vocab_rows
    columns = offset + lax.broadcasted_iota(jnp.int32, (1, vocab_rows), 1)
    onehot = (targets[:, None] == columns).astype(jnp.float32)
    residue = weights / row_total[:, None] - onehot
    partial_grad = lax.dot_general(
        residue,
        tokens.astype(jnp.float32),
        (((0,), (0,)), ((), ())),
        precision=lax.Precision.HIGHEST,
        preferred_element_type=jnp.float32,
    )
    gradient = lax.psum_scatter(partial_grad, "rep", scatter_dimension=1, tiled=True)
    new_hessian = decay_rate * hessian + (1.0 - decay_rate) * gradient * gradient
    step = jnp.clip(momentum / (clip_scale * new_hessian), -1.0, 1.0)
    return (new_hessian, step)


def xor_permute(x, axis, size, bits):
    return lax.ppermute(x, axis, [(i, i ^ bits) for i in range(size)])


def gather_pieces(hidden, sizes):
    reps, shards, group = sizes
    rows = hidden.shape[0]
    half = rows // 2
    side = lax.axis_index("tp") % 2
    rep, shard = lax.axis_index("rep"), lax.axis_index("fsdp")
    mine = lax.dynamic_slice_in_dim(hidden, side * half, half, 0)

    arrived = {(0, 0): mine}
    for j in range(1, reps):
        arrived[(j, 0)] = xor_permute(mine, "rep", reps, j)
    for k in range(1, shards):
        arrived[(0, k)] = xor_permute(mine, "fsdp", shards, k)
        for j in range(1, reps):
            arrived[(j, k)] = xor_permute(arrived[(0, k)], "rep", reps, j)
    pieces, starts = [hidden], [(rep * shards + shard) * rows]
    for (j, k), piece in arrived.items():
        if (j, k) == (0, 0):
            continue
        first = ((rep ^ j) * shards + (shard ^ k)) * rows
        pieces.append(piece)
        starts.append(first + side * half)
        pieces.append(xor_permute(piece, "tp", group, 1))
        starts.append(first + (1 - side) * half)
    return pieces, jnp.stack(starts).astype(jnp.int32)


def copy_pieces(starts, pieces, tokens, sem, columns=None):
    copies = []
    for i, piece in enumerate(pieces):
        rows = piece.shape[0]
        first = pl.multiple_of(starts[i], rows)
        source = piece if columns is None else piece.at[:, columns]
        copies.append(
            pltpu.make_async_copy(source, tokens.at[pl.ds(first, rows), :], sem.at[i])
        )
    for copy in copies:
        copy.start()
    for copy in copies:
        copy.wait()


def logits_kernel(count, starts, weight, *refs):
    pieces, (logits, peak, total), (tokens, sem) = refs[:count], refs[count:count + 3], refs[count + 3:]

    @pl.when(pl.program_id(0) == 0)
    def _():
        copy_pieces(starts, pieces, tokens, sem)
        peak[...] = jnp.full_like(peak, -jnp.inf)
        total[...] = jnp.zeros_like(total)

    block = lax.dot_general(
        weight[...], tokens[...], (((1,), (1,)), ((), ())), preferred_element_type=jnp.float32
    )
    logits[...] = block
    before = peak[...]
    now = jnp.maximum(before, jnp.max(block, axis=0, keepdims=True))
    total[...] = total[...] * jnp.exp(before - now) + jnp.sum(
        jnp.exp(block - now), axis=0, keepdims=True
    )
    peak[...] = now


def update_kernel(count, starts, place, stats, logits, hessian, momentum, *refs):
    pieces, (new_hessian, step), (tokens, sem) = refs[:count], refs[count:count + 2], refs[count + 2:]
    rows, columns = hessian.shape

    @pl.when(pl.program_id(0) == 0)
    def _():
        first = pl.multiple_of(place[1], LANE)
        copy_pieces(starts, pieces, tokens, sem, pl.ds(first, columns))

    peak, inverse, target = stats[0:1, :], 1.0 / stats[1:2, :], stats[2:3, :].astype(jnp.int32)
    block = logits[...]
    own = place[0] + pl.program_id(0) * rows + lax.broadcasted_iota(jnp.int32, block.shape, 0)
    onehot = jnp.where(own == target, 1.0, 0.0)
    residue = jnp.exp(block - peak) * inverse - onehot
    high = residue.astype(jnp.bfloat16)
    low = (residue - high.astype(jnp.float32)).astype(jnp.bfloat16)
    dims = (((1,), (0,)), ((), ()))
    gradient = lax.dot_general(high, tokens[...], dims, preferred_element_type=jnp.float32)
    gradient += lax.dot_general(low, tokens[...], dims, preferred_element_type=jnp.float32)
    fresh = decay_rate * hessian[...] + (1.0 - decay_rate) * gradient * gradient
    new_hessian[...] = fresh
    step[...] = jnp.clip(momentum[...] / (clip_scale * fresh), -1.0, 1.0)


def local(sizes, hidden, labels, weight, hessian, momentum):
    reps, shards, group = sizes
    vocab_rows, depth = weight.shape
    rows, columns = hidden.shape[0], hessian.shape[1]
    count_tokens = reps * shards * rows
    rep, shard = lax.axis_index("rep"), lax.axis_index("fsdp")

    pieces, starts = gather_pieces(hidden, sizes)
    count = len(pieces)

    block = min(256, vocab_rows)
    smem = pl.BlockSpec(memory_space=pltpu.SMEM)
    anywhere = pl.BlockSpec(memory_space=pl.ANY)
    whole = lambda shape: pl.BlockSpec(shape, lambda i: (0, 0))
    logits, peak, total = pl.pallas_call(
        functools.partial(logits_kernel, count),
        grid=(vocab_rows // block,),
        in_specs=[smem, pl.BlockSpec((block, depth), lambda i: (i, 0))] + [anywhere] * count,
        out_specs=[
            pl.BlockSpec((block, count_tokens), lambda i: (i, 0)),
            whole((1, count_tokens)),
            whole((1, count_tokens)),
        ],
        out_shape=[
            jax.ShapeDtypeStruct((vocab_rows, count_tokens), jnp.float32),
            jax.ShapeDtypeStruct((1, count_tokens), jnp.float32),
            jax.ShapeDtypeStruct((1, count_tokens), jnp.float32),
        ],
        scratch_shapes=[
            pltpu.VMEM((count_tokens, depth), jnp.bfloat16),
            pltpu.SemaphoreType.DMA((count,)),
        ],
        compiler_params=pltpu.CompilerParams(vmem_limit_bytes=VMEM_BYTES),
        cost_estimate=pl.CostEstimate(
            flops=2 * vocab_rows * depth * count_tokens,
            bytes_accessed=2 * vocab_rows * depth,
            transcendentals=vocab_rows * count_tokens,
        ),
        name="logits",
    )(starts, weight, *pieces)

    target = lax.dynamic_update_slice_in_dim(
        jnp.zeros((count_tokens,), jnp.float32),
        labels.astype(jnp.float32),
        (rep * shards + shard) * rows,
        0,
    )
    for bits in (1 << b for b in range(reps.bit_length() - 1)):
        target = target + xor_permute(target, "rep", reps, bits)
    stats = jnp.concatenate([peak, total, target[None]], axis=0)
    rounds = [("tp", group, 1 << b) for b in range(group.bit_length() - 1)]
    rounds += [("fsdp", shards, 1 << b) for b in range(shards.bit_length() - 1)]
    for axis, size, bits in rounds:
        other = xor_permute(stats, axis, size, bits)
        top = jnp.maximum(stats[0], other[0])
        full = stats[1] * jnp.exp(stats[0] - top) + other[1] * jnp.exp(other[0] - top)
        label = stats[2] + other[2] if axis == "fsdp" else stats[2]
        stats = jnp.stack([top, full, label])

    place = jnp.stack(
        [lax.axis_index(("fsdp", "tp")) * vocab_rows, rep * columns]
    ).astype(jnp.int32)
    block = min(128, vocab_rows)
    tile = pl.BlockSpec((block, columns), lambda i: (i, 0))
    return pl.pallas_call(
        functools.partial(update_kernel, count),
        grid=(vocab_rows // block,),
        in_specs=[
            smem,
            smem,
            whole((3, count_tokens)),
            pl.BlockSpec((block, count_tokens), lambda i: (i, 0)),
            tile,
            tile,
        ]
        + [anywhere] * count,
        out_specs=[tile, tile],
        out_shape=[jax.ShapeDtypeStruct((vocab_rows, columns), jnp.float32)] * 2,
        scratch_shapes=[
            pltpu.VMEM((count_tokens, columns), jnp.bfloat16),
            pltpu.SemaphoreType.DMA((count,)),
        ],
        compiler_params=pltpu.CompilerParams(vmem_limit_bytes=VMEM_BYTES),
        cost_estimate=pl.CostEstimate(
            flops=4 * vocab_rows * columns * count_tokens,
            bytes_accessed=16 * vocab_rows * columns,
            transcendentals=vocab_rows * count_tokens,
        ),
        name="update",
    )(starts, place, stats, logits, hessian, momentum, *pieces)


def power_of_two(n):
    return n & (n - 1) == 0


def solution(mesh):
    placed = (
        P(("rep", "fsdp"), None),
        P(("rep", "fsdp")),
        P(("fsdp", "tp"), None),
        P(("fsdp", "tp"), "rep"),
        P(("fsdp", "tp"), "rep"),
    )
    sizes = tuple(mesh.shape[name] for name in ("rep", "fsdp", "tp"))

    def body(hidden, labels, weight, hessian, momentum):
        tokens = sizes[0] * sizes[1] * hidden.shape[0]
        fits = (
            all(power_of_two(n) for n in sizes)
            and sizes[0] > 1
            and sizes[2] > 1
            and sizes[0] * sizes[1] <= 16
            and hidden.shape[0] % 32 == 0
            and weight.shape[0] % 128 == 0
            and hessian.shape[1] % LANE == 0
            and tokens * hidden.shape[1] * 2 <= 8 * 1024 * 1024
        )
        if fits:
            return local(sizes, hidden, labels, weight, hessian, momentum)
        return local_large(hidden, labels, weight, hessian, momentum)

    return jax.shard_map(
        body,
        mesh=mesh,
        in_specs=placed,
        out_specs=(P(("fsdp", "tp"), "rep"), P(("fsdp", "tp"), "rep")),
        check_vma=False,
    )
```

```python
import functools

import jax
import jax.numpy as jnp
from jax import lax
from jax.experimental import pallas as pl
from jax.experimental.pallas import tpu as pltpu
from jax.sharding import PartitionSpec as P

decay_rate = 0.99
clip_scale = 0.05


LANE = 128
MIB = 1024 * 1024


def local_large(hidden_states, labels, head_weight, hessian, momentum):
    vocab_rows = head_weight.shape[0]
    tokens, targets = (
        lax.all_gather(hidden_states, "fsdp", axis=0, tiled=True),
        lax.all_gather(labels, "fsdp", axis=0, tiled=True),
    )
    logits = lax.dot_general(
        tokens, head_weight, (((1,), (1,)), ((), ())), preferred_element_type=jnp.float32
    )
    local_max = jnp.max(logits, axis=1)
    row_max = lax.pmax(local_max, ("fsdp", "tp"))
    weights = jnp.exp(logits - row_max[:, None])
    row_total = lax.psum(jnp.sum(weights, axis=1), ("fsdp", "tp"))
    offset = lax.axis_index(("fsdp", "tp")) * vocab_rows
    columns = offset + lax.broadcasted_iota(jnp.int32, (1, vocab_rows), 1)
    onehot = (targets[:, None] == columns).astype(jnp.float32)
    residue = weights / row_total[:, None] - onehot
    partial_grad = lax.dot_general(
        residue,
        tokens.astype(jnp.float32),
        (((0,), (0,)), ((), ())),
        precision=lax.Precision.HIGHEST,
        preferred_element_type=jnp.float32,
    )
    gradient = lax.psum_scatter(partial_grad, "rep", scatter_dimension=1, tiled=True)
    new_hessian = decay_rate * hessian + (1.0 - decay_rate) * gradient * gradient
    step = jnp.clip(momentum / (clip_scale * new_hessian), -1.0, 1.0)
    return (new_hessian, step)


def xor_permute(x, axis, size, bits):
    return lax.ppermute(x, axis, [(i, i ^ bits) for i in range(size)])


def after(x, *others):
    return lax.optimization_barrier((x,) + others)[0]


def vmem_specs(n):
    return [pl.BlockSpec(memory_space=pltpu.VMEM)] * n


def position():
    member = lax.axis_index("tp")
    return lax.axis_index("fsdp"), lax.rem(member, 2), lax.rem(lax.div(member, 2), 2)


def cut_kernel(hidden, near, far):
    half, quarter = near.shape[0], far.shape[0]
    _, side, part = position()
    near[...] = hidden[pl.ds(pl.multiple_of(side * half, half), half), :]
    first = pl.multiple_of(side * half + part * quarter, quarter)
    far[...] = hidden[pl.ds(first, quarter), :]


def join_kernel(count, *refs):
    joined = refs[-1]
    at = 0
    for piece in refs[:count]:
        joined[at:at + piece.shape[0], :] = piece[...]
        at += piece.shape[0]


def begin_gather(hidden, sizes):
    reps, shards, _ = sizes
    rows, depth = hidden.shape
    near, far = pl.pallas_call(
        cut_kernel,
        in_specs=vmem_specs(1),
        out_specs=vmem_specs(2),
        out_shape=[
            jax.ShapeDtypeStruct((rows // 2, depth), hidden.dtype),
            jax.ShapeDtypeStruct((rows // 4, depth), hidden.dtype),
        ],
        compiler_params=pltpu.CompilerParams(vmem_limit_bytes=4 * MIB),
        name="cut",
    )(hidden)
    own = {j: xor_permute(near, "rep", reps, j) for j in range(1, reps)}
    parts = [xor_permute(far, "fsdp", shards, k) for k in range(2, shards)]
    beside = xor_permute(near, "fsdp", shards, 1)
    return own, [after(x, *own.values()) for x in parts], beside


def finish_gather(hidden, own, parts, beside, sizes, consume):
    reps, shards, group = sizes
    distant = range(2, shards)
    joined = pl.pallas_call(
        functools.partial(join_kernel, len(parts)),
        in_specs=vmem_specs(len(parts)) + [],
        out_specs=pl.BlockSpec(memory_space=pltpu.VMEM),
        out_shape=jax.ShapeDtypeStruct(
            (len(parts) * parts[0].shape[0], hidden.shape[1]), hidden.dtype
        ),
        compiler_params=pltpu.CompilerParams(vmem_limit_bytes=4 * MIB),
        name="join",
    )(*parts)

    def both_sides(x, segments):
        there = xor_permute(x, "tp", group, 1)
        other = [(k, 1, part) for k, _, part in segments]
        return [(x, segments), (there, other)]

    def members(pair, mixed, across):
        found = both_sides(pair, [(1, 0, None)])
        found += both_sides(mixed, [(k, 0, 0) for k in distant])
        return found + both_sides(across, [(k, 0, 1) for k in distant])

    theirs = {}
    for j in range(1, reps):
        mixed = xor_permute(joined, "rep", reps, j)
        pair = xor_permute(after(beside, mixed), "rep", reps, j)
        theirs[j] = both_sides(own[j], [(0, 0, None)]), pair, mixed
    across = xor_permute(joined, "tp", group, 2)
    token = consume([(hidden, [(0, None, None)])] + members(beside, joined, across))
    for j, (first, pair, mixed) in theirs.items():
        across = xor_permute(mixed, "tp", group, 2)
        token = consume(first + members(after(pair, token), mixed, after(across, token)))


def logits_kernel(segments, block_rows, column_axis, previous, weight, *refs):
    count = len(segments)
    pieces, earlier, target = refs[:count], refs[count:count + previous], refs[count + previous]
    logits, stats, kept, tokens = refs[count + previous + 1:]
    width, columns = tokens.shape[0], kept.shape[1]
    done = previous * width

    @pl.when(pl.program_id(0) == 0)
    def _():
        shard, side, part = position()
        for piece, places in zip(pieces, segments):
            size = piece.shape[0] // len(places)
            for i, (k, other_side, other_part) in enumerate(places):
                first = (shard ^ k) * block_rows
                if other_side is not None:
                    first += (side ^ other_side) * (block_rows // 2)
                if other_part is not None:
                    first += (part ^ other_part) * (block_rows // 4)
                first = pl.multiple_of(first, size)
                tokens[pl.ds(first, size), :] = piece[i * size:(i + 1) * size, :]
        first = pl.multiple_of(lax.axis_index(column_axis) * columns, LANE)
        kept[...] = tokens[:, pl.ds(first, columns)]
        for i, piece in enumerate(earlier):
            stats[:, i * width:(i + 1) * width] = piece[:, i * width:]
        stats[0:1, done:] = jnp.full((1, width), -jnp.inf, jnp.float32)
        stats[1:2, done:] = jnp.zeros((1, width), jnp.float32)
        stats[2:3, done:] = target[...]

    block = lax.dot_general(
        weight[...], tokens[...], (((1,), (1,)), ((), ())), preferred_element_type=jnp.float32
    )
    rows = block.shape[0]
    logits[pl.ds(pl.multiple_of(pl.program_id(0) * rows, rows), rows), :] = block
    before = stats[0:1, done:]
    now = jnp.maximum(before, jnp.max(block, axis=0, keepdims=True))
    stats[1:2, done:] = stats[1:2, done:] * jnp.exp(before - now) + jnp.sum(
        jnp.exp(block - now), axis=0, keepdims=True
    )
    stats[0:1, done:] = now


def logits_of(pieces, earlier, target, weight, columns, block_rows):
    vocab_rows, depth = weight.shape
    arrays = [x for x, _ in pieces]
    segments = tuple(tuple(places) for _, places in pieces)
    tokens = sum(x.shape[0] for x in arrays)
    block = min(512, vocab_rows)
    return pl.pallas_call(
        functools.partial(logits_kernel, segments, block_rows, "rep", len(earlier)),
        grid=(vocab_rows // block,),
        in_specs=[pl.BlockSpec((block, depth), lambda i: (i, 0))]
        + vmem_specs(len(arrays) + len(earlier) + 1),
        out_specs=vmem_specs(3),
        out_shape=[
            jax.ShapeDtypeStruct((vocab_rows, tokens), jnp.float32),
            jax.ShapeDtypeStruct((3, tokens * (1 + len(earlier))), jnp.float32),
            jax.ShapeDtypeStruct((tokens, columns), jnp.bfloat16),
        ],
        scratch_shapes=[pltpu.VMEM((tokens, depth), jnp.bfloat16)],
        compiler_params=pltpu.CompilerParams(vmem_limit_bytes=48 * MIB),
        cost_estimate=pl.CostEstimate(
            flops=2 * vocab_rows * depth * tokens,
            bytes_accessed=2 * vocab_rows * depth,
            transcendentals=vocab_rows * tokens,
        ),
        name="logits",
    )(weight, *arrays, *earlier, target)


def merge_kernel(labels_too, mine, other, merged):
    top = jnp.maximum(mine[0:1, :], other[0:1, :])
    merged[0:1, :] = top
    merged[1:2, :] = mine[1:2, :] * jnp.exp(mine[0:1, :] - top) + other[1:2, :] * jnp.exp(
        other[0:1, :] - top
    )
    merged[2:3, :] = mine[2:3, :] + other[2:3, :] if labels_too else mine[2:3, :]


def merge(stats, other, labels_too):
    return pl.pallas_call(
        functools.partial(merge_kernel, labels_too),
        in_specs=vmem_specs(2),
        out_specs=pl.BlockSpec(memory_space=pltpu.VMEM),
        out_shape=jax.ShapeDtypeStruct(stats.shape, stats.dtype),
        compiler_params=pltpu.CompilerParams(vmem_limit_bytes=MIB),
        name="merge",
    )(stats, other)


def update_kernel(groups, stats, *refs):
    logits, tokens = refs[:groups], refs[groups:2 * groups]
    hessian, momentum, new_hessian, step = refs[2 * groups:]
    rows = new_hessian.shape[0]
    base = pl.multiple_of(pl.program_id(0) * rows, rows)
    span = pl.ds(base, rows)
    width = logits[0].shape[1]
    first = lax.axis_index(("fsdp", "tp")) * logits[0].shape[0] + base
    peak, inverse, target = stats[0:1, :], 1.0 / stats[1:2, :], stats[2:3, :].astype(jnp.int32)
    gradient = None
    for j in range(groups):
        cols = slice(j * width, (j + 1) * width)
        block = logits[j][span, :]
        own = first + lax.broadcasted_iota(jnp.int32, block.shape, 0)
        onehot = jnp.where(own == target[:, cols], 1.0, 0.0)
        residue = jnp.exp(block - peak[:, cols]) * inverse[:, cols] - onehot
        high = residue.astype(jnp.bfloat16)
        low = (residue - high.astype(jnp.float32)).astype(jnp.bfloat16)
        for term in (high, low):
            term = lax.dot_general(
                term, tokens[j][...], (((1,), (0,)), ((), ())), preferred_element_type=jnp.float32
            )
            gradient = term if gradient is None else gradient + term
    fresh = decay_rate * hessian[...] + (1.0 - decay_rate) * gradient * gradient
    new_hessian[...] = fresh
    step[...] = jnp.clip(momentum[...] / (clip_scale * fresh), -1.0, 1.0)


def local(sizes, hidden, labels, weight, hessian, momentum):
    reps, shards, group = sizes
    vocab_rows = weight.shape[0]
    rows, columns = hidden.shape[0], hessian.shape[1]
    width = shards * rows

    own, parts, beside = begin_gather(hidden, sizes)
    mine = lax.dynamic_update_slice_in_dim(
        jnp.zeros((1, width), jnp.float32),
        labels.astype(jnp.float32)[None],
        lax.axis_index("fsdp") * rows,
        1,
    )
    targets = [mine] + [xor_permute(mine, "rep", reps, j) for j in range(1, reps)]
    logits, kept, stats = [], [], []

    def consume(pieces):
        target = targets[len(logits)]
        block, found, columns_kept = logits_of(pieces, stats, target, weight, columns, rows)
        logits.append(block)
        kept.append(columns_kept)
        stats.append(found)
        return found

    finish_gather(hidden, own, parts, beside, sizes, consume)
    stats = stats[-1]
    rounds = [("tp", group, 1 << b) for b in range(group.bit_length() - 1)]
    rounds += [("fsdp", shards, 1 << b) for b in range(shards.bit_length() - 1)]
    for axis, size, bits in rounds:
        stats = merge(stats, xor_permute(stats, axis, size, bits), axis == "fsdp")

    block = min(256, vocab_rows)
    tile = pl.BlockSpec((block, columns), lambda i: (i, 0))
    return pl.pallas_call(
        functools.partial(update_kernel, reps),
        grid=(vocab_rows // block,),
        in_specs=vmem_specs(2 * reps + 1) + [tile, tile],
        out_specs=[tile, tile],
        out_shape=[jax.ShapeDtypeStruct((vocab_rows, columns), jnp.float32)] * 2,
        compiler_params=pltpu.CompilerParams(vmem_limit_bytes=40 * MIB),
        cost_estimate=pl.CostEstimate(
            flops=4 * vocab_rows * columns * width * reps,
            bytes_accessed=16 * vocab_rows * columns,
            transcendentals=vocab_rows * width * reps,
        ),
        name="update",
    )(stats, *logits, *kept, hessian, momentum)


def power_of_two(n):
    return n & (n - 1) == 0


def solution(mesh):
    placed = (
        P(("rep", "fsdp"), None),
        P(("rep", "fsdp")),
        P(("fsdp", "tp"), None),
        P(("fsdp", "tp"), "rep"),
        P(("fsdp", "tp"), "rep"),
    )
    sizes = tuple(mesh.shape[name] for name in ("rep", "fsdp", "tp"))

    def body(hidden, labels, weight, hessian, momentum):
        tokens = sizes[0] * sizes[1] * hidden.shape[0]
        fits = (
            all(power_of_two(n) for n in sizes)
            and sizes[1] > 2
            and sizes[2] > 2
            and sizes[0] * sizes[1] <= 8
            and hidden.shape[0] % 64 == 0
            and sizes[1] * hidden.shape[0] % LANE == 0
            and weight.shape[0] % 512 == 0
            and hessian.shape[1] % LANE == 0
            and tokens * hidden.shape[1] * 2 <= 4 * 1024 * 1024
            and 8 * hessian.size <= 32 * 1024 * 1024
        )
        if fits:
            return local(sizes, hidden, labels, weight, hessian, momentum)
        return local_large(hidden, labels, weight, hessian, momentum)

    return jax.shard_map(
        body,
        mesh=mesh,
        in_specs=placed,
        out_specs=(P(("fsdp", "tp"), "rep"), P(("fsdp", "tp"), "rep")),
        check_vma=False,
    )
```

```python
import functools

import jax
import jax.numpy as jnp
from jax import lax
from jax.experimental import pallas as pl
from jax.experimental.pallas import tpu as pltpu
from jax.sharding import PartitionSpec as P

decay_rate = 0.99
clip_scale = 0.05


LANE = 128
MIB = 1024 * 1024
MERGE_FLOPS = 4 * 10**9


def local_large(hidden_states, labels, head_weight, hessian, momentum):
    vocab_rows = head_weight.shape[0]
    tokens, targets = (
        lax.all_gather(hidden_states, "fsdp", axis=0, tiled=True),
        lax.all_gather(labels, "fsdp", axis=0, tiled=True),
    )
    logits = lax.dot_general(
        tokens, head_weight, (((1,), (1,)), ((), ())), preferred_element_type=jnp.float32
    )
    local_max = jnp.max(logits, axis=1)
    row_max = lax.pmax(local_max, ("fsdp", "tp"))
    weights = jnp.exp(logits - row_max[:, None])
    row_total = lax.psum(jnp.sum(weights, axis=1), ("fsdp", "tp"))
    offset = lax.axis_index(("fsdp", "tp")) * vocab_rows
    columns = offset + lax.broadcasted_iota(jnp.int32, (1, vocab_rows), 1)
    onehot = (targets[:, None] == columns).astype(jnp.float32)
    residue = weights / row_total[:, None] - onehot
    partial_grad = lax.dot_general(
        residue,
        tokens.astype(jnp.float32),
        (((0,), (0,)), ((), ())),
        precision=lax.Precision.HIGHEST,
        preferred_element_type=jnp.float32,
    )
    gradient = lax.psum_scatter(partial_grad, "rep", scatter_dimension=1, tiled=True)
    new_hessian = decay_rate * hessian + (1.0 - decay_rate) * gradient * gradient
    step = jnp.clip(momentum / (clip_scale * new_hessian), -1.0, 1.0)
    return (new_hessian, step)


def xor_permute(x, axis, size, bits):
    return lax.ppermute(x, axis, [(i, i ^ bits) for i in range(size)])


def after(x, *others):
    return lax.optimization_barrier((x,) + others)[0]


def vmem_specs(n):
    return [pl.BlockSpec(memory_space=pltpu.VMEM)] * n


def position():
    member = lax.axis_index("tp")
    return lax.axis_index("fsdp"), lax.rem(member, 2), lax.rem(lax.div(member, 2), 2)


def cut_kernel(hidden, near, far):
    half, quarter = near.shape[0], far.shape[0]
    _, side, part = position()
    near[...] = hidden[pl.ds(pl.multiple_of(side * half, half), half), :]
    first = pl.multiple_of(side * half + part * quarter, quarter)
    far[...] = hidden[pl.ds(first, quarter), :]


def join_kernel(count, *refs):
    joined = refs[-1]
    at = 0
    for piece in refs[:count]:
        joined[at:at + piece.shape[0], :] = piece[...]
        at += piece.shape[0]


def begin_gather(hidden, sizes):
    reps, shards, _ = sizes
    rows, depth = hidden.shape
    near, far = pl.pallas_call(
        cut_kernel,
        in_specs=vmem_specs(1),
        out_specs=vmem_specs(2),
        out_shape=[
            jax.ShapeDtypeStruct((rows // 2, depth), hidden.dtype),
            jax.ShapeDtypeStruct((rows // 4, depth), hidden.dtype),
        ],
        compiler_params=pltpu.CompilerParams(vmem_limit_bytes=4 * MIB),
        name="cut",
    )(hidden)
    own = {j: xor_permute(near, "rep", reps, j) for j in range(1, reps)}
    parts = [xor_permute(far, "fsdp", shards, k) for k in range(2, shards)]
    beside = xor_permute(near, "fsdp", shards, 1)
    return own, [after(x, *own.values()) for x in parts], beside


def finish_gather(hidden, own, parts, beside, sizes, consume):
    reps, shards, group = sizes
    distant = range(2, shards)
    joined = pl.pallas_call(
        functools.partial(join_kernel, len(parts)),
        in_specs=vmem_specs(len(parts)) + [],
        out_specs=pl.BlockSpec(memory_space=pltpu.VMEM),
        out_shape=jax.ShapeDtypeStruct(
            (len(parts) * parts[0].shape[0], hidden.shape[1]), hidden.dtype
        ),
        compiler_params=pltpu.CompilerParams(vmem_limit_bytes=4 * MIB),
        name="join",
    )(*parts)

    def both_sides(x, segments):
        there = xor_permute(x, "tp", group, 1)
        other = [(k, 1, part) for k, _, part in segments]
        return [(x, segments), (there, other)]

    def members(pair, mixed, across):
        found = both_sides(pair, [(1, 0, None)])
        found += both_sides(mixed, [(k, 0, 0) for k in distant])
        return found + both_sides(across, [(k, 0, 1) for k in distant])

    theirs = {}
    for j in range(1, reps):
        mixed = xor_permute(joined, "rep", reps, j)
        pair = xor_permute(after(beside, mixed), "rep", reps, j)
        theirs[j] = both_sides(own[j], [(0, 0, None)]), pair, mixed
    across = xor_permute(joined, "tp", group, 2)
    token = consume([(hidden, [(0, None, None)])] + members(beside, joined, across))
    for j, (first, pair, mixed) in theirs.items():
        across = xor_permute(mixed, "tp", group, 2)
        token = consume(first + members(after(pair, token), mixed, after(across, token)))


def logits_kernel(segments, block_rows, column_axis, previous, weight, *refs):
    count = len(segments)
    pieces, earlier, target = refs[:count], refs[count:count + previous], refs[count + previous]
    logits, stats, kept, tokens = refs[count + previous + 1:]
    width, columns = tokens.shape[0], kept.shape[1]
    done = previous * width

    @pl.when(pl.program_id(0) == 0)
    def _():
        shard, side, part = position()
        for piece, places in zip(pieces, segments):
            size = piece.shape[0] // len(places)
            for i, (k, other_side, other_part) in enumerate(places):
                first = (shard ^ k) * block_rows
                if other_side is not None:
                    first += (side ^ other_side) * (block_rows // 2)
                if other_part is not None:
                    first += (part ^ other_part) * (block_rows // 4)
                first = pl.multiple_of(first, size)
                tokens[pl.ds(first, size), :] = piece[i * size:(i + 1) * size, :]
        first = pl.multiple_of(lax.axis_index(column_axis) * columns, LANE)
        kept[...] = tokens[:, pl.ds(first, columns)]
        for i, piece in enumerate(earlier):
            stats[:, i * width:(i + 1) * width] = piece[:, i * width:]
        stats[0:1, done:] = jnp.full((1, width), -jnp.inf, jnp.float32)
        stats[1:2, done:] = jnp.zeros((1, width), jnp.float32)
        stats[2:3, done:] = target[...]

    block = lax.dot_general(
        weight[...], tokens[...], (((1,), (1,)), ((), ())), preferred_element_type=jnp.float32
    )
    rows = block.shape[0]
    logits[pl.ds(pl.multiple_of(pl.program_id(0) * rows, rows), rows), :] = block
    before = stats[0:1, done:]
    now = jnp.maximum(before, jnp.max(block, axis=0, keepdims=True))
    stats[1:2, done:] = stats[1:2, done:] * jnp.exp(before - now) + jnp.sum(
        jnp.exp(block - now), axis=0, keepdims=True
    )
    stats[0:1, done:] = now


def logits_of(pieces, earlier, target, weight, columns, block_rows):
    vocab_rows, depth = weight.shape
    arrays = [x for x, _ in pieces]
    segments = tuple(tuple(places) for _, places in pieces)
    tokens = sum(x.shape[0] for x in arrays)
    block = min(512, vocab_rows)
    return pl.pallas_call(
        functools.partial(logits_kernel, segments, block_rows, "rep", len(earlier)),
        grid=(vocab_rows // block,),
        in_specs=[pl.BlockSpec((block, depth), lambda i: (i, 0))]
        + vmem_specs(len(arrays) + len(earlier) + 1),
        out_specs=vmem_specs(3),
        out_shape=[
            jax.ShapeDtypeStruct((vocab_rows, tokens), jnp.float32),
            jax.ShapeDtypeStruct((3, tokens * (1 + len(earlier))), jnp.float32),
            jax.ShapeDtypeStruct((tokens, columns), jnp.bfloat16),
        ],
        scratch_shapes=[pltpu.VMEM((tokens, depth), jnp.bfloat16)],
        compiler_params=pltpu.CompilerParams(vmem_limit_bytes=48 * MIB),
        cost_estimate=pl.CostEstimate(
            flops=2 * vocab_rows * depth * tokens,
            bytes_accessed=2 * vocab_rows * depth,
            transcendentals=vocab_rows * tokens,
        ),
        name="logits",
    )(weight, *arrays, *earlier, target)


def merge_kernel(labels_too, mine, other, merged):
    top = jnp.maximum(mine[0:1, :], other[0:1, :])
    merged[0:1, :] = top
    merged[1:2, :] = mine[1:2, :] * jnp.exp(mine[0:1, :] - top) + other[1:2, :] * jnp.exp(
        other[0:1, :] - top
    )
    merged[2:3, :] = mine[2:3, :] + other[2:3, :] if labels_too else mine[2:3, :]


def merge(stats, other, labels_too):
    return pl.pallas_call(
        functools.partial(merge_kernel, labels_too),
        in_specs=vmem_specs(2),
        out_specs=pl.BlockSpec(memory_space=pltpu.VMEM),
        out_shape=jax.ShapeDtypeStruct(stats.shape, stats.dtype),
        compiler_params=pltpu.CompilerParams(vmem_limit_bytes=MIB),
        cost_estimate=pl.CostEstimate(flops=MERGE_FLOPS, bytes_accessed=0, transcendentals=0),
        name="merge",
    )(stats, other)


def update_kernel(groups, stats, *refs):
    logits, tokens = refs[:groups], refs[groups:2 * groups]
    hessian, momentum, new_hessian, step = refs[2 * groups:]
    rows = new_hessian.shape[0]
    base = pl.multiple_of(pl.program_id(0) * rows, rows)
    span = pl.ds(base, rows)
    width = logits[0].shape[1]
    first = lax.axis_index(("fsdp", "tp")) * logits[0].shape[0] + base
    peak, inverse, target = stats[0:1, :], 1.0 / stats[1:2, :], stats[2:3, :].astype(jnp.int32)
    gradient = None
    for j in range(groups):
        cols = slice(j * width, (j + 1) * width)
        block = logits[j][span, :]
        own = first + lax.broadcasted_iota(jnp.int32, block.shape, 0)
        onehot = jnp.where(own == target[:, cols], 1.0, 0.0)
        residue = jnp.exp(block - peak[:, cols]) * inverse[:, cols] - onehot
        high = residue.astype(jnp.bfloat16)
        low = (residue - high.astype(jnp.float32)).astype(jnp.bfloat16)
        for term in (high, low):
            term = lax.dot_general(
                term, tokens[j][...], (((1,), (0,)), ((), ())), preferred_element_type=jnp.float32
            )
            gradient = term if gradient is None else gradient + term
    fresh = decay_rate * hessian[span, :] + (1.0 - decay_rate) * gradient * gradient
    new_hessian[...] = fresh
    step[...] = jnp.clip(momentum[span, :] / (clip_scale * fresh), -1.0, 1.0)


def local(sizes, hidden, labels, weight, hessian, momentum):
    reps, shards, group = sizes
    vocab_rows = weight.shape[0]
    rows, columns = hidden.shape[0], hessian.shape[1]
    width = shards * rows

    own, parts, beside = begin_gather(hidden, sizes)
    mine = lax.dynamic_update_slice_in_dim(
        jnp.zeros((1, width), jnp.float32),
        labels.astype(jnp.float32)[None],
        lax.axis_index("fsdp") * rows,
        1,
    )
    targets = [mine] + [xor_permute(mine, "rep", reps, j) for j in range(1, reps)]
    logits, kept, stats = [], [], []

    def consume(pieces):
        target = targets[len(logits)]
        block, found, columns_kept = logits_of(pieces, stats, target, weight, columns, rows)
        logits.append(block)
        kept.append(columns_kept)
        stats.append(found)
        return found

    finish_gather(hidden, own, parts, beside, sizes, consume)
    stats = stats[-1]
    rounds = [("tp", group, 1 << b) for b in range(group.bit_length() - 1)]
    rounds += [("fsdp", shards, 1 << b) for b in range(shards.bit_length() - 1)]
    for axis, size, bits in rounds:
        stats = merge(stats, xor_permute(stats, axis, size, bits), axis == "fsdp")

    block = min(256, vocab_rows)
    tile = pl.BlockSpec((block, columns), lambda i: (i, 0))
    return pl.pallas_call(
        functools.partial(update_kernel, reps),
        grid=(vocab_rows // block,),
        in_specs=vmem_specs(2 * reps + 3),
        out_specs=[tile, tile],
        out_shape=[jax.ShapeDtypeStruct((vocab_rows, columns), jnp.float32)] * 2,
        compiler_params=pltpu.CompilerParams(vmem_limit_bytes=13 * MIB),
        cost_estimate=pl.CostEstimate(
            flops=0,
            bytes_accessed=16 * vocab_rows * columns,
            transcendentals=vocab_rows * width * reps,
        ),
        name="update",
    )(stats, *logits, *kept, hessian, momentum)


def power_of_two(n):
    return n & (n - 1) == 0


def solution(mesh):
    placed = (
        P(("rep", "fsdp"), None),
        P(("rep", "fsdp")),
        P(("fsdp", "tp"), None),
        P(("fsdp", "tp"), "rep"),
        P(("fsdp", "tp"), "rep"),
    )
    sizes = tuple(mesh.shape[name] for name in ("rep", "fsdp", "tp"))

    def body(hidden, labels, weight, hessian, momentum):
        tokens = sizes[0] * sizes[1] * hidden.shape[0]
        fits = (
            all(power_of_two(n) for n in sizes)
            and sizes[1] > 2
            and sizes[2] > 2
            and sizes[0] * sizes[1] <= 8
            and hidden.shape[0] % 64 == 0
            and sizes[1] * hidden.shape[0] % LANE == 0
            and weight.shape[0] % 512 == 0
            and hessian.shape[1] % LANE == 0
            and tokens * hidden.shape[1] * 2 <= 4 * 1024 * 1024
            and 8 * hessian.size <= 32 * 1024 * 1024
        )
        if fits:
            return local(sizes, hidden, labels, weight, hessian, momentum)
        return local_large(hidden, labels, weight, hessian, momentum)

    return jax.shard_map(
        body,
        mesh=mesh,
        in_specs=placed,
        out_specs=(P(("fsdp", "tp"), "rep"), P(("fsdp", "tp"), "rep")),
        check_vma=False,
    )
```

```python
import functools

import jax
import jax.numpy as jnp
from jax import lax
from jax.experimental import pallas as pl
from jax.experimental.pallas import tpu as pltpu
from jax.sharding import PartitionSpec as P

decay_rate = 0.99
clip_scale = 0.05


LANE = 128
MIB = 1024 * 1024
MERGE_FLOPS = 4 * 10**9
JOIN_FLOPS = 5 * 10**9


def local_large(hidden_states, labels, head_weight, hessian, momentum):
    vocab_rows = head_weight.shape[0]
    tokens, targets = (
        lax.all_gather(hidden_states, "fsdp", axis=0, tiled=True),
        lax.all_gather(labels, "fsdp", axis=0, tiled=True),
    )
    logits = lax.dot_general(
        tokens, head_weight, (((1,), (1,)), ((), ())), preferred_element_type=jnp.float32
    )
    local_max = jnp.max(logits, axis=1)
    row_max = lax.pmax(local_max, ("fsdp", "tp"))
    weights = jnp.exp(logits - row_max[:, None])
    row_total = lax.psum(jnp.sum(weights, axis=1), ("fsdp", "tp"))
    offset = lax.axis_index(("fsdp", "tp")) * vocab_rows
    columns = offset + lax.broadcasted_iota(jnp.int32, (1, vocab_rows), 1)
    onehot = (targets[:, None] == columns).astype(jnp.float32)
    residue = weights / row_total[:, None] - onehot
    partial_grad = lax.dot_general(
        residue,
        tokens.astype(jnp.float32),
        (((0,), (0,)), ((), ())),
        precision=lax.Precision.HIGHEST,
        preferred_element_type=jnp.float32,
    )
    gradient = lax.psum_scatter(partial_grad, "rep", scatter_dimension=1, tiled=True)
    new_hessian = decay_rate * hessian + (1.0 - decay_rate) * gradient * gradient
    step = jnp.clip(momentum / (clip_scale * new_hessian), -1.0, 1.0)
    return (new_hessian, step)


def xor_permute(x, axis, size, bits):
    return lax.ppermute(x, axis, [(i, i ^ bits) for i in range(size)])


def after(x, *others):
    return lax.optimization_barrier((x,) + others)[0]


def vmem_specs(n):
    return [pl.BlockSpec(memory_space=pltpu.VMEM)] * n


def position():
    member = lax.axis_index("tp")
    return lax.axis_index("fsdp"), lax.rem(member, 2), lax.rem(lax.div(member, 2), 2)


def cut_kernel(hidden, own, near, far):
    half, quarter = near.shape[0], far.shape[0]
    own[...] = hidden[...]
    _, side, part = position()
    near[...] = hidden[pl.ds(pl.multiple_of(side * half, half), half), :]
    first = pl.multiple_of(side * half + part * quarter, quarter)
    far[...] = hidden[pl.ds(first, quarter), :]


def label_kernel(labels, placed):
    shard, _, _ = position()
    values = labels[...].astype(jnp.float32)
    rows = values.shape[1]
    for k in range(placed.shape[1] // rows):
        placed[:, k * rows:(k + 1) * rows] = jnp.where(shard == k, values, 0.0)


def join_kernel(count, *refs):
    joined = refs[-1]
    at = 0
    for piece in refs[:count]:
        joined[at:at + piece.shape[0], :] = piece[...]
        at += piece.shape[0]


def begin_gather(hidden, sizes):
    reps, shards, _ = sizes
    rows, depth = hidden.shape
    kept, near, far = pl.pallas_call(
        cut_kernel,
        in_specs=vmem_specs(1),
        out_specs=vmem_specs(3),
        out_shape=[
            jax.ShapeDtypeStruct((rows, depth), hidden.dtype),
            jax.ShapeDtypeStruct((rows // 2, depth), hidden.dtype),
            jax.ShapeDtypeStruct((rows // 4, depth), hidden.dtype),
        ],
        compiler_params=pltpu.CompilerParams(vmem_limit_bytes=4 * MIB),
        name="cut",
    )(hidden)
    own = {j: xor_permute(near, "rep", reps, j) for j in range(1, reps)}
    parts = [xor_permute(far, "fsdp", shards, k) for k in range(2, shards)]
    beside = xor_permute(near, "fsdp", shards, 1)
    return kept, own, parts, beside


def finish_gather(hidden, own, parts, beside, sizes, consume):
    reps, shards, group = sizes
    distant = range(2, shards)
    joined = pl.pallas_call(
        functools.partial(join_kernel, len(parts)),
        in_specs=vmem_specs(len(parts)) + [],
        out_specs=pl.BlockSpec(memory_space=pltpu.VMEM),
        out_shape=jax.ShapeDtypeStruct(
            (len(parts) * parts[0].shape[0], hidden.shape[1]), hidden.dtype
        ),
        compiler_params=pltpu.CompilerParams(vmem_limit_bytes=4 * MIB),
        cost_estimate=pl.CostEstimate(flops=JOIN_FLOPS, bytes_accessed=0, transcendentals=0),
        name="join",
    )(*parts)

    def both_sides(x, segments):
        there = xor_permute(x, "tp", group, 1)
        other = [(k, 1, part) for k, _, part in segments]
        return [(x, segments), (there, other)]

    def members(pair, mixed, across):
        found = both_sides(pair, [(1, 0, None)])
        found += both_sides(mixed, [(k, 0, 0) for k in distant])
        return found + both_sides(across, [(k, 0, 1) for k in distant])

    theirs = {}
    for j in range(1, reps):
        mixed = xor_permute(joined, "rep", reps, j)
        pair = xor_permute(after(beside, mixed), "rep", reps, j)
        theirs[j] = both_sides(own[j], [(0, 0, None)]), pair, mixed
    across = xor_permute(joined, "tp", group, 2)
    token = consume([(hidden, [(0, None, None)])] + members(beside, joined, across))
    for j, (first, pair, mixed) in theirs.items():
        across = xor_permute(mixed, "tp", group, 2)
        token = consume(first + members(after(pair, token), mixed, after(across, token)))


def logits_kernel(segments, block_rows, column_axis, previous, weight, *refs):
    count = len(segments)
    pieces, earlier, target = refs[:count], refs[count:count + previous], refs[count + previous]
    logits, stats, kept, tokens = refs[count + previous + 1:]
    width, columns = tokens.shape[0], kept.shape[1]
    done = previous * width

    @pl.when(pl.program_id(0) == 0)
    def _():
        shard, side, part = position()
        for piece, places in zip(pieces, segments):
            size = piece.shape[0] // len(places)
            for i, (k, other_side, other_part) in enumerate(places):
                first = (shard ^ k) * block_rows
                if other_side is not None:
                    first += (side ^ other_side) * (block_rows // 2)
                if other_part is not None:
                    first += (part ^ other_part) * (block_rows // 4)
                first = pl.multiple_of(first, size)
                tokens[pl.ds(first, size), :] = piece[i * size:(i + 1) * size, :]
        first = pl.multiple_of(lax.axis_index(column_axis) * columns, LANE)
        kept[...] = tokens[:, pl.ds(first, columns)]
        for i, piece in enumerate(earlier):
            stats[:, i * width:(i + 1) * width] = piece[:, i * width:]
        stats[0:1, done:] = jnp.full((1, width), -jnp.inf, jnp.float32)
        stats[1:2, done:] = jnp.zeros((1, width), jnp.float32)
        stats[2:3, done:] = target[...]

    block = lax.dot_general(
        weight[...], tokens[...], (((1,), (1,)), ((), ())), preferred_element_type=jnp.float32
    )
    rows = block.shape[0]
    logits[pl.ds(pl.multiple_of(pl.program_id(0) * rows, rows), rows), :] = block
    before = stats[0:1, done:]
    now = jnp.maximum(before, jnp.max(block, axis=0, keepdims=True))
    stats[1:2, done:] = stats[1:2, done:] * jnp.exp(before - now) + jnp.sum(
        jnp.exp(block - now), axis=0, keepdims=True
    )
    stats[0:1, done:] = now


def logits_of(pieces, earlier, target, weight, columns, block_rows):
    vocab_rows, depth = weight.shape
    arrays = [x for x, _ in pieces]
    segments = tuple(tuple(places) for _, places in pieces)
    tokens = sum(x.shape[0] for x in arrays)
    block = min(512, vocab_rows)
    return pl.pallas_call(
        functools.partial(logits_kernel, segments, block_rows, "rep", len(earlier)),
        grid=(vocab_rows // block,),
        in_specs=[pl.BlockSpec((block, depth), lambda i: (i, 0))]
        + vmem_specs(len(arrays) + len(earlier) + 1),
        out_specs=vmem_specs(3),
        out_shape=[
            jax.ShapeDtypeStruct((vocab_rows, tokens), jnp.float32),
            jax.ShapeDtypeStruct((3, tokens * (1 + len(earlier))), jnp.float32),
            jax.ShapeDtypeStruct((tokens, columns), jnp.bfloat16),
        ],
        scratch_shapes=[pltpu.VMEM((tokens, depth), jnp.bfloat16)],
        compiler_params=pltpu.CompilerParams(vmem_limit_bytes=14 * MIB),
        cost_estimate=pl.CostEstimate(
            flops=2 * vocab_rows * depth * tokens,
            bytes_accessed=2 * vocab_rows * depth,
            transcendentals=vocab_rows * tokens,
        ),
        name="logits",
    )(weight, *arrays, *earlier, target)


def merge_kernel(labels_too, mine, other, merged):
    top = jnp.maximum(mine[0:1, :], other[0:1, :])
    merged[0:1, :] = top
    merged[1:2, :] = mine[1:2, :] * jnp.exp(mine[0:1, :] - top) + other[1:2, :] * jnp.exp(
        other[0:1, :] - top
    )
    merged[2:3, :] = mine[2:3, :] + other[2:3, :] if labels_too else mine[2:3, :]


def merge(stats, other, labels_too):
    return pl.pallas_call(
        functools.partial(merge_kernel, labels_too),
        in_specs=vmem_specs(2),
        out_specs=pl.BlockSpec(memory_space=pltpu.VMEM),
        out_shape=jax.ShapeDtypeStruct(stats.shape, stats.dtype),
        compiler_params=pltpu.CompilerParams(vmem_limit_bytes=MIB),
        cost_estimate=pl.CostEstimate(flops=MERGE_FLOPS, bytes_accessed=0, transcendentals=0),
        name="merge",
    )(stats, other)


def update_kernel(groups, stats, *refs):
    logits, tokens = refs[:groups], refs[groups:2 * groups]
    hessian, momentum, new_hessian, step = refs[2 * groups:]
    rows = new_hessian.shape[0]
    base = pl.multiple_of(pl.program_id(0) * rows, rows)
    span = pl.ds(base, rows)
    width = logits[0].shape[1]
    first = lax.axis_index(("fsdp", "tp")) * logits[0].shape[0] + base
    peak, inverse, target = stats[0:1, :], 1.0 / stats[1:2, :], stats[2:3, :].astype(jnp.int32)
    gradient = None
    for j in range(groups):
        cols = slice(j * width, (j + 1) * width)
        block = logits[j][span, :]
        own = first + lax.broadcasted_iota(jnp.int32, block.shape, 0)
        onehot = jnp.where(own == target[:, cols], 1.0, 0.0)
        residue = jnp.exp(block - peak[:, cols]) * inverse[:, cols] - onehot
        high = residue.astype(jnp.bfloat16)
        low = (residue - high.astype(jnp.float32)).astype(jnp.bfloat16)
        for term in (high, low):
            term = lax.dot_general(
                term, tokens[j][...], (((1,), (0,)), ((), ())), preferred_element_type=jnp.float32
            )
            gradient = term if gradient is None else gradient + term
    fresh = decay_rate * hessian[span, :] + (1.0 - decay_rate) * gradient * gradient
    new_hessian[...] = fresh
    step[...] = jnp.clip(momentum[span, :] / (clip_scale * fresh), -1.0, 1.0)


def local(sizes, hidden, labels, weight, hessian, momentum):
    reps, shards, group = sizes
    vocab_rows = weight.shape[0]
    rows, columns = hidden.shape[0], hessian.shape[1]
    width = shards * rows

    hidden, own, parts, beside = begin_gather(hidden, sizes)
    mine = pl.pallas_call(
        label_kernel,
        in_specs=vmem_specs(1),
        out_specs=pl.BlockSpec(memory_space=pltpu.VMEM),
        out_shape=jax.ShapeDtypeStruct((1, width), jnp.float32),
        compiler_params=pltpu.CompilerParams(vmem_limit_bytes=MIB),
        name="label",
    )(labels[None])
    targets = [mine] + [xor_permute(mine, "rep", reps, j) for j in range(1, reps)]
    parts = [after(x, *own.values(), *targets) for x in parts]
    logits, kept, stats = [], [], []

    def consume(pieces):
        target = targets[len(logits)]
        block, found, columns_kept = logits_of(pieces, stats, target, weight, columns, rows)
        logits.append(block)
        kept.append(columns_kept)
        stats.append(found)
        return found

    finish_gather(hidden, own, parts, beside, sizes, consume)
    stats = stats[-1]
    rounds = [("tp", group, 1 << b) for b in range(group.bit_length() - 1)]
    rounds += [("fsdp", shards, 1 << b) for b in range(shards.bit_length() - 1)]
    for axis, size, bits in rounds:
        stats = merge(stats, xor_permute(stats, axis, size, bits), axis == "fsdp")

    block = min(256, vocab_rows)
    tile = pl.BlockSpec((block, columns), lambda i: (i, 0))
    return pl.pallas_call(
        functools.partial(update_kernel, reps),
        grid=(vocab_rows // block,),
        in_specs=vmem_specs(2 * reps + 3),
        out_specs=[tile, tile],
        out_shape=[jax.ShapeDtypeStruct((vocab_rows, columns), jnp.float32)] * 2,
        compiler_params=pltpu.CompilerParams(vmem_limit_bytes=13 * MIB),
        cost_estimate=pl.CostEstimate(
            flops=0,
            bytes_accessed=16 * vocab_rows * columns,
            transcendentals=vocab_rows * width * reps,
        ),
        name="update",
    )(stats, *logits, *kept, hessian, momentum)


def power_of_two(n):
    return n & (n - 1) == 0


def solution(mesh):
    placed = (
        P(("rep", "fsdp"), None),
        P(("rep", "fsdp")),
        P(("fsdp", "tp"), None),
        P(("fsdp", "tp"), "rep"),
        P(("fsdp", "tp"), "rep"),
    )
    sizes = tuple(mesh.shape[name] for name in ("rep", "fsdp", "tp"))

    def body(hidden, labels, weight, hessian, momentum):
        tokens = sizes[0] * sizes[1] * hidden.shape[0]
        fits = (
            all(power_of_two(n) for n in sizes)
            and sizes[1] > 2
            and sizes[2] > 2
            and sizes[0] * sizes[1] <= 8
            and hidden.shape[0] % 64 == 0
            and sizes[1] * hidden.shape[0] % LANE == 0
            and weight.shape[0] % 512 == 0
            and hessian.shape[1] % LANE == 0
            and tokens * hidden.shape[1] * 2 <= 4 * 1024 * 1024
            and 8 * hessian.size <= 32 * 1024 * 1024
        )
        if fits:
            return local(sizes, hidden, labels, weight, hessian, momentum)
        return local_large(hidden, labels, weight, hessian, momentum)

    return jax.shard_map(
        body,
        mesh=mesh,
        in_specs=placed,
        out_specs=(P(("fsdp", "tp"), "rep"), P(("fsdp", "tp"), "rep")),
        check_vma=False,
    )
```

```python
import functools

import jax
import jax.numpy as jnp
from jax import lax
from jax.experimental import pallas as pl
from jax.experimental.pallas import tpu as pltpu
from jax.sharding import PartitionSpec as P

decay_rate = 0.99
clip_scale = 0.05


LANE = 128
MIB = 1024 * 1024
MERGE_FLOPS = 3 * 10**9
JOIN_FLOPS = 5 * 10**9


def local_large(hidden_states, labels, head_weight, hessian, momentum):
    vocab_rows = head_weight.shape[0]
    tokens, targets = (
        lax.all_gather(hidden_states, "fsdp", axis=0, tiled=True),
        lax.all_gather(labels, "fsdp", axis=0, tiled=True),
    )
    logits = lax.dot_general(
        tokens, head_weight, (((1,), (1,)), ((), ())), preferred_element_type=jnp.float32
    )
    local_max = jnp.max(logits, axis=1)
    row_max = lax.pmax(local_max, ("fsdp", "tp"))
    weights = jnp.exp(logits - row_max[:, None])
    row_total = lax.psum(jnp.sum(weights, axis=1), ("fsdp", "tp"))
    offset = lax.axis_index(("fsdp", "tp")) * vocab_rows
    columns = offset + lax.broadcasted_iota(jnp.int32, (1, vocab_rows), 1)
    onehot = (targets[:, None] == columns).astype(jnp.float32)
    residue = weights / row_total[:, None] - onehot
    partial_grad = lax.dot_general(
        residue,
        tokens.astype(jnp.float32),
        (((0,), (0,)), ((), ())),
        precision=lax.Precision.HIGHEST,
        preferred_element_type=jnp.float32,
    )
    gradient = lax.psum_scatter(partial_grad, "rep", scatter_dimension=1, tiled=True)
    new_hessian = decay_rate * hessian + (1.0 - decay_rate) * gradient * gradient
    step = jnp.clip(momentum / (clip_scale * new_hessian), -1.0, 1.0)
    return (new_hessian, step)


def xor_permute(x, axis, size, bits):
    return lax.ppermute(x, axis, [(i, i ^ bits) for i in range(size)])


def after(x, *others):
    return lax.optimization_barrier((x,) + others)[0]


def vmem_specs(n):
    return [pl.BlockSpec(memory_space=pltpu.VMEM)] * n


def position():
    member = lax.axis_index("tp")
    return lax.axis_index("fsdp"), lax.rem(member, 2), lax.rem(lax.div(member, 2), 2)


def cut_kernel(hidden, own, near, far):
    half, quarter = near.shape[0], far.shape[0]
    own[...] = hidden[...]
    _, side, part = position()
    near[...] = hidden[pl.ds(pl.multiple_of(side * half, half), half), :]
    first = pl.multiple_of(side * half + part * quarter, quarter)
    far[...] = hidden[pl.ds(first, quarter), :]


def label_kernel(labels, placed):
    shard, _, _ = position()
    values = labels[...].astype(jnp.float32)
    rows = values.shape[1]
    for k in range(placed.shape[1] // rows):
        placed[:, k * rows:(k + 1) * rows] = jnp.where(shard == k, values, 0.0)


def join_kernel(count, *refs):
    joined = refs[-1]
    at = 0
    for piece in refs[:count]:
        joined[at:at + piece.shape[0], :] = piece[...]
        at += piece.shape[0]


def begin_gather(hidden, sizes):
    reps, shards, _ = sizes
    rows, depth = hidden.shape
    kept, near, far = pl.pallas_call(
        cut_kernel,
        in_specs=vmem_specs(1),
        out_specs=vmem_specs(3),
        out_shape=[
            jax.ShapeDtypeStruct((rows, depth), hidden.dtype),
            jax.ShapeDtypeStruct((rows // 2, depth), hidden.dtype),
            jax.ShapeDtypeStruct((rows // 4, depth), hidden.dtype),
        ],
        compiler_params=pltpu.CompilerParams(vmem_limit_bytes=4 * MIB),
        name="cut",
    )(hidden)
    own = {j: xor_permute(near, "rep", reps, j) for j in range(1, reps)}
    parts = [xor_permute(far, "fsdp", shards, k) for k in range(2, shards)]
    beside = xor_permute(near, "fsdp", shards, 1)
    return kept, own, parts, beside


def finish_gather(hidden, own, parts, beside, sizes, consume):
    reps, shards, group = sizes
    distant = range(2, shards)
    joined = pl.pallas_call(
        functools.partial(join_kernel, len(parts)),
        in_specs=vmem_specs(len(parts)) + [],
        out_specs=pl.BlockSpec(memory_space=pltpu.VMEM),
        out_shape=jax.ShapeDtypeStruct(
            (len(parts) * parts[0].shape[0], hidden.shape[1]), hidden.dtype
        ),
        compiler_params=pltpu.CompilerParams(vmem_limit_bytes=4 * MIB),
        cost_estimate=pl.CostEstimate(flops=JOIN_FLOPS, bytes_accessed=0, transcendentals=0),
        name="join",
    )(*parts)

    def both_sides(x, segments):
        there = xor_permute(x, "tp", group, 1)
        other = [(k, 1, part) for k, _, part in segments]
        return [(x, segments), (there, other)]

    def members(pair, mixed, across):
        found = both_sides(pair, [(1, 0, None)])
        found += both_sides(mixed, [(k, 0, 0) for k in distant])
        return found + both_sides(across, [(k, 0, 1) for k in distant])

    theirs = {}
    for j in range(1, reps):
        mixed = xor_permute(joined, "rep", reps, j)
        pair = xor_permute(after(beside, mixed), "rep", reps, j)
        theirs[j] = both_sides(own[j], [(0, 0, None)]), pair, mixed
    across = xor_permute(joined, "tp", group, 2)
    token = consume([(hidden, [(0, None, None)])] + members(beside, joined, across))
    for j, (first, pair, mixed) in theirs.items():
        across = xor_permute(mixed, "tp", group, 2)
        token = consume(first + members(after(pair, token), mixed, after(across, token)))


def logits_kernel(segments, block_rows, column_axis, previous, weight, *refs):
    count = len(segments)
    pieces, earlier, target = refs[:count], refs[count:count + previous], refs[count + previous]
    logits, stats, kept, tokens = refs[count + previous + 1:]
    width, columns = tokens.shape[0], kept.shape[1]
    done = previous * width

    @pl.when(pl.program_id(0) == 0)
    def _():
        shard, side, part = position()
        for piece, places in zip(pieces, segments):
            size = piece.shape[0] // len(places)
            for i, (k, other_side, other_part) in enumerate(places):
                first = (shard ^ k) * block_rows
                if other_side is not None:
                    first += (side ^ other_side) * (block_rows // 2)
                if other_part is not None:
                    first += (part ^ other_part) * (block_rows // 4)
                first = pl.multiple_of(first, size)
                tokens[pl.ds(first, size), :] = piece[i * size:(i + 1) * size, :]
        first = pl.multiple_of(lax.axis_index(column_axis) * columns, LANE)
        kept[...] = tokens[:, pl.ds(first, columns)]
        for i, piece in enumerate(earlier):
            stats[:, i * width:(i + 1) * width] = piece[:, i * width:]
        stats[0:1, done:] = jnp.full((1, width), -jnp.inf, jnp.float32)
        stats[1:2, done:] = jnp.zeros((1, width), jnp.float32)
        stats[2:3, done:] = target[...]

    block = lax.dot_general(
        weight[...], tokens[...], (((1,), (1,)), ((), ())), preferred_element_type=jnp.float32
    )
    rows = block.shape[0]
    logits[pl.ds(pl.multiple_of(pl.program_id(0) * rows, rows), rows), :] = block
    before = stats[0:1, done:]
    now = jnp.maximum(before, jnp.max(block, axis=0, keepdims=True))
    stats[1:2, done:] = stats[1:2, done:] * jnp.exp(before - now) + jnp.sum(
        jnp.exp(block - now), axis=0, keepdims=True
    )
    stats[0:1, done:] = now


def logits_of(pieces, earlier, target, weight, columns, block_rows):
    vocab_rows, depth = weight.shape
    arrays = [x for x, _ in pieces]
    segments = tuple(tuple(places) for _, places in pieces)
    tokens = sum(x.shape[0] for x in arrays)
    block = min(512, vocab_rows)
    return pl.pallas_call(
        functools.partial(logits_kernel, segments, block_rows, "rep", len(earlier)),
        grid=(vocab_rows // block,),
        in_specs=[pl.BlockSpec((block, depth), lambda i: (i, 0))]
        + vmem_specs(len(arrays) + len(earlier) + 1),
        out_specs=vmem_specs(3),
        out_shape=[
            jax.ShapeDtypeStruct((vocab_rows, tokens), jnp.float32),
            jax.ShapeDtypeStruct((3, tokens * (1 + len(earlier))), jnp.float32),
            jax.ShapeDtypeStruct((tokens, columns), jnp.bfloat16),
        ],
        scratch_shapes=[pltpu.VMEM((tokens, depth), jnp.bfloat16)],
        compiler_params=pltpu.CompilerParams(vmem_limit_bytes=14 * MIB),
        cost_estimate=pl.CostEstimate(
            flops=2 * vocab_rows * depth * tokens,
            bytes_accessed=2 * vocab_rows * depth,
            transcendentals=vocab_rows * tokens,
        ),
        name="logits",
    )(weight, *arrays, *earlier, target)


def merge_kernel(labels_too, *refs):
    parts, merged = refs[:-1], refs[-1]
    top = parts[0][0:1, :]
    for part in parts[1:]:
        top = jnp.maximum(top, part[0:1, :])
    full, label = 0.0, parts[0][2:3, :]
    for part in parts:
        full += part[1:2, :] * jnp.exp(part[0:1, :] - top)
    if labels_too:
        for part in parts[1:]:
            label += part[2:3, :]
    merged[0:1, :], merged[1:2, :], merged[2:3, :] = top, full, label


def merge(labels_too, flops, *parts):
    stats = parts[0]
    return pl.pallas_call(
        functools.partial(merge_kernel, labels_too),
        in_specs=vmem_specs(len(parts)),
        out_specs=pl.BlockSpec(memory_space=pltpu.VMEM),
        out_shape=jax.ShapeDtypeStruct(stats.shape, stats.dtype),
        compiler_params=pltpu.CompilerParams(vmem_limit_bytes=MIB),
        cost_estimate=pl.CostEstimate(flops=flops, bytes_accessed=0, transcendentals=0),
        name="merge",
    )(*parts)


def update_kernel(groups, stats, *refs):
    logits, tokens = refs[:groups], refs[groups:2 * groups]
    hessian, momentum, new_hessian, step = refs[2 * groups:]
    rows = new_hessian.shape[0]
    base = pl.multiple_of(pl.program_id(0) * rows, rows)
    span = pl.ds(base, rows)
    width = logits[0].shape[1]
    first = lax.axis_index(("fsdp", "tp")) * logits[0].shape[0] + base
    peak, inverse, target = stats[0:1, :], 1.0 / stats[1:2, :], stats[2:3, :].astype(jnp.int32)
    gradient = None
    for j in range(groups):
        cols = slice(j * width, (j + 1) * width)
        block = logits[j][span, :]
        own = first + lax.broadcasted_iota(jnp.int32, block.shape, 0)
        onehot = jnp.where(own == target[:, cols], 1.0, 0.0)
        residue = jnp.exp(block - peak[:, cols]) * inverse[:, cols] - onehot
        high = residue.astype(jnp.bfloat16)
        low = (residue - high.astype(jnp.float32)).astype(jnp.bfloat16)
        for term in (high, low):
            term = lax.dot_general(
                term, tokens[j][...], (((1,), (0,)), ((), ())), preferred_element_type=jnp.float32
            )
            gradient = term if gradient is None else gradient + term
    fresh = decay_rate * hessian[span, :] + (1.0 - decay_rate) * gradient * gradient
    new_hessian[...] = fresh
    step[...] = jnp.clip(momentum[span, :] / (clip_scale * fresh), -1.0, 1.0)


def local(sizes, hidden, labels, weight, hessian, momentum):
    reps, shards, group = sizes
    vocab_rows = weight.shape[0]
    rows, columns = hidden.shape[0], hessian.shape[1]
    width = shards * rows

    hidden, own, parts, beside = begin_gather(hidden, sizes)
    mine = pl.pallas_call(
        label_kernel,
        in_specs=vmem_specs(1),
        out_specs=pl.BlockSpec(memory_space=pltpu.VMEM),
        out_shape=jax.ShapeDtypeStruct((1, width), jnp.float32),
        compiler_params=pltpu.CompilerParams(vmem_limit_bytes=MIB),
        name="label",
    )(after(labels[None], *own.values()))
    targets = [mine] + [xor_permute(mine, "rep", reps, j) for j in range(1, reps)]
    parts = [after(x, *own.values(), *targets) for x in parts]
    logits, kept, stats = [], [], []

    def consume(pieces):
        target = targets[len(logits)]
        block, found, columns_kept = logits_of(pieces, stats, target, weight, columns, rows)
        logits.append(block)
        kept.append(columns_kept)
        stats.append(found)
        return found

    finish_gather(hidden, own, parts, beside, sizes, consume)
    stats = stats[-1]
    for bits in (1 << b for b in range(group.bit_length() - 1)):
        stats = merge(False, MERGE_FLOPS, stats, xor_permute(stats, "tp", group, bits))
    others = [xor_permute(stats, "fsdp", shards, k) for k in range(1, shards)]
    stats = merge(True, 2 * MERGE_FLOPS, stats, *others)

    block = min(256, vocab_rows)
    tile = pl.BlockSpec((block, columns), lambda i: (i, 0))
    return pl.pallas_call(
        functools.partial(update_kernel, reps),
        grid=(vocab_rows // block,),
        in_specs=vmem_specs(2 * reps + 3),
        out_specs=[tile, tile],
        out_shape=[jax.ShapeDtypeStruct((vocab_rows, columns), jnp.float32)] * 2,
        compiler_params=pltpu.CompilerParams(vmem_limit_bytes=13 * MIB),
        cost_estimate=pl.CostEstimate(
            flops=0,
            bytes_accessed=16 * vocab_rows * columns,
            transcendentals=vocab_rows * width * reps,
        ),
        name="update",
    )(stats, *logits, *kept, hessian, momentum)


def power_of_two(n):
    return n & (n - 1) == 0


def solution(mesh):
    placed = (
        P(("rep", "fsdp"), None),
        P(("rep", "fsdp")),
        P(("fsdp", "tp"), None),
        P(("fsdp", "tp"), "rep"),
        P(("fsdp", "tp"), "rep"),
    )
    sizes = tuple(mesh.shape[name] for name in ("rep", "fsdp", "tp"))

    def body(hidden, labels, weight, hessian, momentum):
        tokens = sizes[0] * sizes[1] * hidden.shape[0]
        fits = (
            all(power_of_two(n) for n in sizes)
            and sizes[1] > 2
            and sizes[2] > 2
            and sizes[0] * sizes[1] <= 8
            and hidden.shape[0] % 64 == 0
            and sizes[1] * hidden.shape[0] % LANE == 0
            and weight.shape[0] % 512 == 0
            and hessian.shape[1] % LANE == 0
            and tokens * hidden.shape[1] * 2 <= 4 * 1024 * 1024
            and 8 * hessian.size <= 32 * 1024 * 1024
        )
        if fits:
            return local(sizes, hidden, labels, weight, hessian, momentum)
        return local_large(hidden, labels, weight, hessian, momentum)

    return jax.shard_map(
        body,
        mesh=mesh,
        in_specs=placed,
        out_specs=(P(("fsdp", "tp"), "rep"), P(("fsdp", "tp"), "rep")),
        check_vma=False,
    )
```

```python
import functools
import math

import jax
import jax.numpy as jnp
from jax import lax
from jax.experimental import pallas as pl
from jax.experimental.pallas import tpu as pltpu
from jax.sharding import PartitionSpec as P

decay_rate = 0.99
clip_scale = 0.05


LANE = 128
MIB = 1024 * 1024
MERGE_FLOPS = 2 * 10**9
JOIN_FLOPS = 5 * 10**9


def local_large(hidden_states, labels, head_weight, hessian, momentum):
    vocab_rows = head_weight.shape[0]
    tokens, targets = (
        lax.all_gather(hidden_states, "fsdp", axis=0, tiled=True),
        lax.all_gather(labels, "fsdp", axis=0, tiled=True),
    )
    logits = lax.dot_general(
        tokens, head_weight, (((1,), (1,)), ((), ())), preferred_element_type=jnp.float32
    )
    local_max = jnp.max(logits, axis=1)
    row_max = lax.pmax(local_max, ("fsdp", "tp"))
    weights = jnp.exp(logits - row_max[:, None])
    row_total = lax.psum(jnp.sum(weights, axis=1), ("fsdp", "tp"))
    offset = lax.axis_index(("fsdp", "tp")) * vocab_rows
    columns = offset + lax.broadcasted_iota(jnp.int32, (1, vocab_rows), 1)
    onehot = (targets[:, None] == columns).astype(jnp.float32)
    residue = weights / row_total[:, None] - onehot
    partial_grad = lax.dot_general(
        residue,
        tokens.astype(jnp.float32),
        (((0,), (0,)), ((), ())),
        precision=lax.Precision.HIGHEST,
        preferred_element_type=jnp.float32,
    )
    gradient = lax.psum_scatter(partial_grad, "rep", scatter_dimension=1, tiled=True)
    new_hessian = decay_rate * hessian + (1.0 - decay_rate) * gradient * gradient
    step = jnp.clip(momentum / (clip_scale * new_hessian), -1.0, 1.0)
    return (new_hessian, step)


def xor_permute(x, axis, size, bits):
    return lax.ppermute(x, axis, [(i, i ^ bits) for i in range(size)])


def after(x, *others):
    return lax.optimization_barrier((x,) + others)[0]


def vmem_specs(n):
    return [pl.BlockSpec(memory_space=pltpu.VMEM)] * n


def position():
    member = lax.axis_index("tp")
    return lax.axis_index("fsdp"), lax.rem(member, 2), lax.rem(lax.div(member, 2), 2)


def cut_kernel(hidden, own, near, far):
    half, quarter = near.shape[0], far.shape[0]
    own[...] = hidden[...]
    _, side, part = position()
    near[...] = hidden[pl.ds(pl.multiple_of(side * half, half), half), :]
    first = pl.multiple_of(side * half + part * quarter, quarter)
    far[...] = hidden[pl.ds(first, quarter), :]


def label_kernel(labels, placed):
    shard, _, _ = position()
    values = labels[...].astype(jnp.float32)
    rows = values.shape[1]
    for k in range(placed.shape[1] // rows):
        placed[:, k * rows:(k + 1) * rows] = jnp.where(shard == k, values, 0.0)


def join_kernel(count, *refs):
    joined = refs[-1]
    at = 0
    for piece in refs[:count]:
        joined[at:at + piece.shape[0], :] = piece[...]
        at += piece.shape[0]


def begin_gather(hidden, sizes):
    reps, shards, _ = sizes
    rows, depth = hidden.shape
    kept, near, far = pl.pallas_call(
        cut_kernel,
        in_specs=vmem_specs(1),
        out_specs=vmem_specs(3),
        out_shape=[
            jax.ShapeDtypeStruct((rows, depth), hidden.dtype),
            jax.ShapeDtypeStruct((rows // 2, depth), hidden.dtype),
            jax.ShapeDtypeStruct((rows // 4, depth), hidden.dtype),
        ],
        compiler_params=pltpu.CompilerParams(vmem_limit_bytes=4 * MIB),
        name="cut",
    )(hidden)
    own = {j: xor_permute(near, "rep", reps, j) for j in range(1, reps)}
    parts = [xor_permute(far, "fsdp", shards, k) for k in range(2, shards)]
    beside = xor_permute(near, "fsdp", shards, 1)
    return kept, own, parts, beside


def finish_gather(hidden, own, parts, beside, sizes, consume):
    reps, shards, group = sizes
    distant = range(2, shards)
    joined = pl.pallas_call(
        functools.partial(join_kernel, len(parts)),
        in_specs=vmem_specs(len(parts)) + [],
        out_specs=pl.BlockSpec(memory_space=pltpu.VMEM),
        out_shape=jax.ShapeDtypeStruct(
            (len(parts) * parts[0].shape[0], hidden.shape[1]), hidden.dtype
        ),
        compiler_params=pltpu.CompilerParams(vmem_limit_bytes=4 * MIB),
        cost_estimate=pl.CostEstimate(flops=JOIN_FLOPS, bytes_accessed=0, transcendentals=0),
        name="join",
    )(*parts)

    def both_sides(x, segments):
        there = xor_permute(x, "tp", group, 1)
        other = [(k, 1, part) for k, _, part in segments]
        return [(x, segments), (there, other)]

    def members(pair, mixed, across):
        found = both_sides(pair, [(1, 0, None)])
        found += both_sides(mixed, [(k, 0, 0) for k in distant])
        return found + both_sides(across, [(k, 0, 1) for k in distant])

    theirs = {}
    for j in range(1, reps):
        mixed = xor_permute(joined, "rep", reps, j)
        pair = xor_permute(after(beside, mixed), "rep", reps, j)
        theirs[j] = both_sides(own[j], [(0, 0, None)]), pair, mixed
    across = xor_permute(joined, "tp", group, 2)
    token = consume([(hidden, [(0, None, None)])] + members(beside, joined, across))
    for j, (first, pair, mixed) in theirs.items():
        across = xor_permute(mixed, "tp", group, 2)
        token = consume(
            first + members(after(pair, token), after(mixed, token), after(across, token))
        )


def logits_kernel(segments, block_rows, column_axis, previous, weight, *refs):
    count = len(segments)
    pieces, earlier, target = refs[:count], refs[count:count + previous], refs[count + previous]
    logits, stats, kept, tokens = refs[count + previous + 1:]
    width, columns = tokens.shape[0], kept.shape[1]
    done = previous * width

    @pl.when(pl.program_id(0) == 0)
    def _():
        shard, side, part = position()
        for piece, places in zip(pieces, segments):
            size = piece.shape[0] // len(places)
            for i, (k, other_side, other_part) in enumerate(places):
                first = (shard ^ k) * block_rows
                if other_side is not None:
                    first += (side ^ other_side) * (block_rows // 2)
                if other_part is not None:
                    first += (part ^ other_part) * (block_rows // 4)
                first = pl.multiple_of(first, size)
                tokens[pl.ds(first, size), :] = piece[i * size:(i + 1) * size, :]
        first = pl.multiple_of(lax.axis_index(column_axis) * columns, LANE)
        kept[...] = tokens[:, pl.ds(first, columns)]
        for i, piece in enumerate(earlier):
            stats[:, i * width:(i + 1) * width] = piece[:, i * width:]
        stats[0:1, done:] = jnp.full((1, width), -jnp.inf, jnp.float32)
        stats[1:2, done:] = jnp.zeros((1, width), jnp.float32)
        stats[2:3, done:] = target[...]

    block = lax.dot_general(
        weight[...], tokens[...], (((1,), (1,)), ((), ())), preferred_element_type=jnp.float32
    )
    rows = block.shape[0]
    logits[pl.ds(pl.multiple_of(pl.program_id(0) * rows, rows), rows), :] = block
    before = stats[0:1, done:]
    now = jnp.maximum(before, jnp.max(block, axis=0, keepdims=True))
    stats[1:2, done:] = stats[1:2, done:] * jnp.exp(before - now) + jnp.sum(
        jnp.exp(block - now), axis=0, keepdims=True
    )
    stats[0:1, done:] = now


def logits_of(pieces, earlier, target, weight, columns, block_rows):
    vocab_rows, depth = weight.shape
    arrays = [x for x, _ in pieces]
    segments = tuple(tuple(places) for _, places in pieces)
    tokens = sum(x.shape[0] for x in arrays)
    block = min(512, vocab_rows)
    return pl.pallas_call(
        functools.partial(logits_kernel, segments, block_rows, "rep", len(earlier)),
        grid=(vocab_rows // block,),
        in_specs=[pl.BlockSpec((block, depth), lambda i: (i, 0))]
        + vmem_specs(len(arrays) + len(earlier) + 1),
        out_specs=vmem_specs(3),
        out_shape=[
            jax.ShapeDtypeStruct((vocab_rows, tokens), jnp.float32),
            jax.ShapeDtypeStruct((3, tokens * (1 + len(earlier))), jnp.float32),
            jax.ShapeDtypeStruct((tokens, columns), jnp.bfloat16),
        ],
        scratch_shapes=[pltpu.VMEM((tokens, depth), jnp.bfloat16)],
        compiler_params=pltpu.CompilerParams(vmem_limit_bytes=14 * MIB),
        cost_estimate=pl.CostEstimate(
            flops=2 * vocab_rows * depth * tokens,
            bytes_accessed=2 * vocab_rows * depth,
            transcendentals=vocab_rows * tokens,
        ),
        name="logits",
    )(weight, *arrays, *earlier, target)


def merge_kernel(labels_too, *refs):
    parts, merged = refs[:-1], refs[-1]
    top = parts[0][0:1, :]
    for part in parts[1:]:
        top = jnp.maximum(top, part[0:1, :])
    full, label = 0.0, parts[0][2:3, :]
    for part in parts:
        full += part[1:2, :] * jnp.exp(part[0:1, :] - top)
    if labels_too:
        for part in parts[1:]:
            label += part[2:3, :]
    merged[0:1, :], merged[1:2, :], merged[2:3, :] = top, full, label


def merge(labels_too, flops, *parts):
    stats = parts[0]
    return pl.pallas_call(
        functools.partial(merge_kernel, labels_too),
        in_specs=vmem_specs(len(parts)),
        out_specs=pl.BlockSpec(memory_space=pltpu.VMEM),
        out_shape=jax.ShapeDtypeStruct(stats.shape, stats.dtype),
        compiler_params=pltpu.CompilerParams(vmem_limit_bytes=MIB),
        cost_estimate=pl.CostEstimate(flops=flops, bytes_accessed=0, transcendentals=0),
        name="merge",
    )(*parts)


def weight_kernel(done, logits, stats, weights):
    width = logits.shape[1]
    weights[...] = jnp.exp(logits[...] - stats[0:1, done:done + width])


def weights_of(logits, stats, done):
    return pl.pallas_call(
        functools.partial(weight_kernel, done),
        in_specs=vmem_specs(2),
        out_specs=pl.BlockSpec(memory_space=pltpu.VMEM),
        out_shape=jax.ShapeDtypeStruct(logits.shape, logits.dtype),
        compiler_params=pltpu.CompilerParams(vmem_limit_bytes=2 * MIB),
        cost_estimate=pl.CostEstimate(flops=10**9, bytes_accessed=0, transcendentals=0),
        name="weights",
    )(logits, stats)


def update_kernel(groups, stats, own_stats, *refs):
    weights, tokens = refs[:groups], refs[groups:2 * groups]
    hessian, momentum, new_hessian, step = refs[2 * groups:]
    rows = new_hessian.shape[0]
    base = pl.multiple_of(pl.program_id(0) * rows, rows)
    span = pl.ds(base, rows)
    width = weights[0].shape[1]
    first = lax.axis_index(("fsdp", "tp")) * weights[0].shape[0] + base
    root = math.sqrt(1.0 - decay_rate)
    factor = root * jnp.exp(own_stats[0:1, :] - stats[0:1, :]) / stats[1:2, :]
    target = stats[2:3, :].astype(jnp.int32)
    gradient = None
    for j in range(groups):
        cols = slice(j * width, (j + 1) * width)
        block = weights[j][span, :]
        own = first + lax.broadcasted_iota(jnp.int32, block.shape, 0)
        onehot = jnp.where(own == target[:, cols], root, 0.0)
        residue = block * factor[:, cols] - onehot
        high = residue.astype(jnp.bfloat16)
        low = (residue - high.astype(jnp.float32)).astype(jnp.bfloat16)
        for term in (high, low):
            term = lax.dot_general(
                term, tokens[j][...], (((1,), (0,)), ((), ())), preferred_element_type=jnp.float32
            )
            gradient = term if gradient is None else gradient + term
    fresh = decay_rate * hessian[span, :] + gradient * gradient
    new_hessian[...] = fresh
    step[...] = jnp.clip(momentum[span, :] / (clip_scale * fresh), -1.0, 1.0)


def local(sizes, hidden, labels, weight, hessian, momentum):
    reps, shards, group = sizes
    vocab_rows = weight.shape[0]
    rows, columns = hidden.shape[0], hessian.shape[1]
    width = shards * rows

    hidden, own, parts, beside = begin_gather(hidden, sizes)
    mine = pl.pallas_call(
        label_kernel,
        in_specs=vmem_specs(1),
        out_specs=pl.BlockSpec(memory_space=pltpu.VMEM),
        out_shape=jax.ShapeDtypeStruct((1, width), jnp.float32),
        compiler_params=pltpu.CompilerParams(vmem_limit_bytes=MIB),
        name="label",
    )(after(labels[None], *own.values()))
    targets = [mine] + [xor_permute(mine, "rep", reps, j) for j in range(1, reps)]
    parts = [after(x, *own.values(), *targets) for x in parts]
    logits, kept, stats = [], [], []

    def consume(pieces):
        target = targets[len(logits)]
        block, found, columns_kept = logits_of(pieces, stats, target, weight, columns, rows)
        logits.append(weights_of(block, found, len(logits) * width))
        kept.append(columns_kept)
        stats.append(found)
        return found

    finish_gather(hidden, own, parts, beside, sizes, consume)
    stats = own_stats = stats[-1]
    for bits in (1 << b for b in range(group.bit_length() - 1)):
        stats = merge(False, MERGE_FLOPS, stats, xor_permute(stats, "tp", group, bits))
    others = [xor_permute(stats, "fsdp", shards, k) for k in range(1, shards)]
    stats = merge(True, 2 * MERGE_FLOPS, stats, *others)

    block = min(256, vocab_rows)
    tile = pl.BlockSpec((block, columns), lambda i: (i, 0))
    return pl.pallas_call(
        functools.partial(update_kernel, reps),
        grid=(vocab_rows // block,),
        in_specs=vmem_specs(2 * reps + 4),
        out_specs=[tile, tile],
        out_shape=[jax.ShapeDtypeStruct((vocab_rows, columns), jnp.float32)] * 2,
        compiler_params=pltpu.CompilerParams(vmem_limit_bytes=13 * MIB),
        cost_estimate=pl.CostEstimate(
            flops=0,
            bytes_accessed=16 * vocab_rows * columns,
            transcendentals=vocab_rows * width * reps,
        ),
        name="update",
    )(stats, own_stats, *logits, *kept, hessian, momentum)


def power_of_two(n):
    return n & (n - 1) == 0


def solution(mesh):
    placed = (
        P(("rep", "fsdp"), None),
        P(("rep", "fsdp")),
        P(("fsdp", "tp"), None),
        P(("fsdp", "tp"), "rep"),
        P(("fsdp", "tp"), "rep"),
    )
    sizes = tuple(mesh.shape[name] for name in ("rep", "fsdp", "tp"))

    def body(hidden, labels, weight, hessian, momentum):
        tokens = sizes[0] * sizes[1] * hidden.shape[0]
        fits = (
            all(power_of_two(n) for n in sizes)
            and sizes[1] > 2
            and sizes[2] > 2
            and sizes[0] * sizes[1] <= 8
            and hidden.shape[0] % 64 == 0
            and sizes[1] * hidden.shape[0] % LANE == 0
            and weight.shape[0] % 512 == 0
            and hessian.shape[1] % LANE == 0
            and tokens * hidden.shape[1] * 2 <= 4 * 1024 * 1024
            and 8 * hessian.size <= 32 * 1024 * 1024
        )
        if fits:
            return local(sizes, hidden, labels, weight, hessian, momentum)
        return local_large(hidden, labels, weight, hessian, momentum)

    return jax.shard_map(
        body,
        mesh=mesh,
        in_specs=placed,
        out_specs=(P(("fsdp", "tp"), "rep"), P(("fsdp", "tp"), "rep")),
        check_vma=False,
    )
```

```python
import functools
import math

import jax
import jax.numpy as jnp
from jax import lax
from jax.experimental import pallas as pl
from jax.experimental.pallas import tpu as pltpu
from jax.sharding import PartitionSpec as P

decay_rate = 0.99
clip_scale = 0.05


LANE = 128
MIB = 1024 * 1024
MERGE_FLOPS = 3 * 10**9
JOIN_FLOPS = 5 * 10**9


def local_large(hidden_states, labels, head_weight, hessian, momentum):
    vocab_rows = head_weight.shape[0]
    tokens, targets = (
        lax.all_gather(hidden_states, "fsdp", axis=0, tiled=True),
        lax.all_gather(labels, "fsdp", axis=0, tiled=True),
    )
    logits = lax.dot_general(
        tokens, head_weight, (((1,), (1,)), ((), ())), preferred_element_type=jnp.float32
    )
    local_max = jnp.max(logits, axis=1)
    row_max = lax.pmax(local_max, ("fsdp", "tp"))
    weights = jnp.exp(logits - row_max[:, None])
    row_total = lax.psum(jnp.sum(weights, axis=1), ("fsdp", "tp"))
    offset = lax.axis_index(("fsdp", "tp")) * vocab_rows
    columns = offset + lax.broadcasted_iota(jnp.int32, (1, vocab_rows), 1)
    onehot = (targets[:, None] == columns).astype(jnp.float32)
    residue = weights / row_total[:, None] - onehot
    partial_grad = lax.dot_general(
        residue,
        tokens.astype(jnp.float32),
        (((0,), (0,)), ((), ())),
        precision=lax.Precision.HIGHEST,
        preferred_element_type=jnp.float32,
    )
    gradient = lax.psum_scatter(partial_grad, "rep", scatter_dimension=1, tiled=True)
    new_hessian = decay_rate * hessian + (1.0 - decay_rate) * gradient * gradient
    step = jnp.clip(momentum / (clip_scale * new_hessian), -1.0, 1.0)
    return (new_hessian, step)


def xor_permute(x, axis, size, bits):
    return lax.ppermute(x, axis, [(i, i ^ bits) for i in range(size)])


def after(x, *others):
    return lax.optimization_barrier((x,) + others)[0]


def vmem_specs(n):
    return [pl.BlockSpec(memory_space=pltpu.VMEM)] * n


def position():
    member = lax.axis_index("tp")
    return lax.axis_index("fsdp"), lax.rem(member, 2), lax.rem(lax.div(member, 2), 2)


def cut_kernel(hidden, own, near, far):
    half, quarter = near.shape[0], far.shape[0]
    own[...] = hidden[...]
    _, side, part = position()
    near[...] = hidden[pl.ds(pl.multiple_of(side * half, half), half), :]
    first = pl.multiple_of(side * half + part * quarter, quarter)
    far[...] = hidden[pl.ds(first, quarter), :]


def label_kernel(labels, placed):
    shard, _, _ = position()
    values = labels[...].astype(jnp.float32)
    rows = values.shape[1]
    for k in range(placed.shape[1] // rows):
        placed[:, k * rows:(k + 1) * rows] = jnp.where(shard == k, values, 0.0)


def join_kernel(count, *refs):
    joined = refs[-1]
    at = 0
    for piece in refs[:count]:
        joined[at:at + piece.shape[0], :] = piece[...]
        at += piece.shape[0]


def begin_gather(hidden, sizes):
    reps, shards, _ = sizes
    rows, depth = hidden.shape
    kept, near, far = pl.pallas_call(
        cut_kernel,
        in_specs=vmem_specs(1),
        out_specs=vmem_specs(3),
        out_shape=[
            jax.ShapeDtypeStruct((rows, depth), hidden.dtype),
            jax.ShapeDtypeStruct((rows // 2, depth), hidden.dtype),
            jax.ShapeDtypeStruct((rows // 4, depth), hidden.dtype),
        ],
        compiler_params=pltpu.CompilerParams(vmem_limit_bytes=4 * MIB),
        name="cut",
    )(hidden)
    own = {j: xor_permute(near, "rep", reps, j) for j in range(1, reps)}
    parts = [xor_permute(far, "fsdp", shards, k) for k in range(2, shards)]
    beside = xor_permute(near, "fsdp", shards, 1)
    return kept, own, parts, beside


def finish_gather(hidden, own, parts, beside, sizes, consume):
    reps, shards, group = sizes
    distant = range(2, shards)
    joined = pl.pallas_call(
        functools.partial(join_kernel, len(parts)),
        in_specs=vmem_specs(len(parts)) + [],
        out_specs=pl.BlockSpec(memory_space=pltpu.VMEM),
        out_shape=jax.ShapeDtypeStruct(
            (len(parts) * parts[0].shape[0], hidden.shape[1]), hidden.dtype
        ),
        compiler_params=pltpu.CompilerParams(vmem_limit_bytes=4 * MIB),
        cost_estimate=pl.CostEstimate(flops=JOIN_FLOPS, bytes_accessed=0, transcendentals=0),
        name="join",
    )(*parts)

    def both_sides(x, segments):
        there = xor_permute(x, "tp", group, 1)
        other = [(k, 1, part) for k, _, part in segments]
        return [(x, segments), (there, other)]

    def members(pair, mixed, across):
        found = both_sides(pair, [(1, 0, None)])
        found += both_sides(mixed, [(k, 0, 0) for k in distant])
        return found + both_sides(across, [(k, 0, 1) for k in distant])

    theirs = {}
    for j in range(1, reps):
        mixed = xor_permute(joined, "rep", reps, j)
        pair = xor_permute(after(beside, mixed), "rep", reps, j)
        theirs[j] = both_sides(own[j], [(0, 0, None)]), pair, mixed
    across = xor_permute(joined, "tp", group, 2)
    token = consume([(hidden, [(0, None, None)])] + members(beside, joined, across))
    for j, (first, pair, mixed) in theirs.items():
        across = xor_permute(mixed, "tp", group, 2)
        token = consume(
            first + members(after(pair, token), mixed, after(across, token))
        )


def logits_kernel(segments, block_rows, column_axis, previous, weight, *refs):
    count = len(segments)
    pieces, earlier, target = refs[:count], refs[count:count + previous], refs[count + previous]
    logits, stats, kept, tokens = refs[count + previous + 1:]
    width, columns = tokens.shape[0], kept.shape[1]
    done = previous * width

    @pl.when(pl.program_id(0) == 0)
    def _():
        shard, side, part = position()
        for piece, places in zip(pieces, segments):
            size = piece.shape[0] // len(places)
            for i, (k, other_side, other_part) in enumerate(places):
                first = (shard ^ k) * block_rows
                if other_side is not None:
                    first += (side ^ other_side) * (block_rows // 2)
                if other_part is not None:
                    first += (part ^ other_part) * (block_rows // 4)
                first = pl.multiple_of(first, size)
                tokens[pl.ds(first, size), :] = piece[i * size:(i + 1) * size, :]
        first = pl.multiple_of(lax.axis_index(column_axis) * columns, LANE)
        kept[...] = tokens[:, pl.ds(first, columns)]
        for i, piece in enumerate(earlier):
            stats[:, i * width:(i + 1) * width] = piece[:, i * width:]
        stats[0:1, done:] = jnp.full((1, width), -jnp.inf, jnp.float32)
        stats[1:2, done:] = jnp.zeros((1, width), jnp.float32)
        stats[2:3, done:] = target[...]

    block = lax.dot_general(
        weight[...], tokens[...], (((1,), (1,)), ((), ())), preferred_element_type=jnp.float32
    )
    rows = block.shape[0]
    logits[pl.ds(pl.multiple_of(pl.program_id(0) * rows, rows), rows), :] = block
    before = stats[0:1, done:]
    now = jnp.maximum(before, jnp.max(block, axis=0, keepdims=True))
    stats[1:2, done:] = stats[1:2, done:] * jnp.exp(before - now) + jnp.sum(
        jnp.exp(block - now), axis=0, keepdims=True
    )
    stats[0:1, done:] = now


def logits_of(pieces, earlier, target, weight, columns, block_rows):
    vocab_rows, depth = weight.shape
    arrays = [x for x, _ in pieces]
    segments = tuple(tuple(places) for _, places in pieces)
    tokens = sum(x.shape[0] for x in arrays)
    block = min(512, vocab_rows)
    return pl.pallas_call(
        functools.partial(logits_kernel, segments, block_rows, "rep", len(earlier)),
        grid=(vocab_rows // block,),
        in_specs=[pl.BlockSpec((block, depth), lambda i: (i, 0))]
        + vmem_specs(len(arrays) + len(earlier) + 1),
        out_specs=vmem_specs(3),
        out_shape=[
            jax.ShapeDtypeStruct((vocab_rows, tokens), jnp.float32),
            jax.ShapeDtypeStruct((3, tokens * (1 + len(earlier))), jnp.float32),
            jax.ShapeDtypeStruct((tokens, columns), jnp.bfloat16),
        ],
        scratch_shapes=[pltpu.VMEM((tokens, depth), jnp.bfloat16)],
        compiler_params=pltpu.CompilerParams(vmem_limit_bytes=14 * MIB),
        cost_estimate=pl.CostEstimate(
            flops=2 * vocab_rows * depth * tokens,
            bytes_accessed=2 * vocab_rows * depth,
            transcendentals=vocab_rows * tokens,
        ),
        name="logits",
    )(weight, *arrays, *earlier, target)


def merge_kernel(labels_too, *refs):
    parts, merged = refs[:-1], refs[-1]
    top = parts[0][0:1, :]
    for part in parts[1:]:
        top = jnp.maximum(top, part[0:1, :])
    full, label = 0.0, parts[0][2:3, :]
    for part in parts:
        full += part[1:2, :] * jnp.exp(part[0:1, :] - top)
    if labels_too:
        for part in parts[1:]:
            label += part[2:3, :]
    merged[0:1, :], merged[1:2, :], merged[2:3, :] = top, full, label


def merge(labels_too, flops, *parts):
    stats = parts[0]
    return pl.pallas_call(
        functools.partial(merge_kernel, labels_too),
        in_specs=vmem_specs(len(parts)),
        out_specs=pl.BlockSpec(memory_space=pltpu.VMEM),
        out_shape=jax.ShapeDtypeStruct(stats.shape, stats.dtype),
        compiler_params=pltpu.CompilerParams(vmem_limit_bytes=MIB),
        cost_estimate=pl.CostEstimate(flops=flops, bytes_accessed=0, transcendentals=0),
        name="merge",
    )(*parts)


def weight_kernel(done, logits, stats, weights):
    width = logits.shape[1]
    weights[...] = jnp.exp(logits[...] - stats[0:1, done:done + width])


def weights_of(logits, stats, done):
    return pl.pallas_call(
        functools.partial(weight_kernel, done),
        in_specs=vmem_specs(2),
        out_specs=pl.BlockSpec(memory_space=pltpu.VMEM),
        out_shape=jax.ShapeDtypeStruct(logits.shape, logits.dtype),
        compiler_params=pltpu.CompilerParams(vmem_limit_bytes=2 * MIB),
        cost_estimate=pl.CostEstimate(flops=100000000, bytes_accessed=0, transcendentals=0),
        name="weights",
    )(logits, stats)


def update_kernel(groups, stats, own_stats, *refs):
    weights, tokens = refs[:groups], refs[groups:2 * groups]
    hessian, momentum, new_hessian, step = refs[2 * groups:]
    rows = new_hessian.shape[0]
    base = pl.multiple_of(pl.program_id(0) * rows, rows)
    span = pl.ds(base, rows)
    width = weights[0].shape[1]
    first = lax.axis_index(("fsdp", "tp")) * weights[0].shape[0] + base
    root = math.sqrt(1.0 - decay_rate)
    factor = root * jnp.exp(own_stats[0:1, :] - stats[0:1, :]) / stats[1:2, :]
    target = stats[2:3, :].astype(jnp.int32)
    gradient = None
    for j in range(groups):
        cols = slice(j * width, (j + 1) * width)
        block = weights[j][span, :]
        own = first + lax.broadcasted_iota(jnp.int32, block.shape, 0)
        onehot = jnp.where(own == target[:, cols], root, 0.0)
        residue = block * factor[:, cols] - onehot
        high = residue.astype(jnp.bfloat16)
        low = (residue - high.astype(jnp.float32)).astype(jnp.bfloat16)
        for term in (high, low):
            term = lax.dot_general(
                term, tokens[j][...], (((1,), (0,)), ((), ())), preferred_element_type=jnp.float32
            )
            gradient = term if gradient is None else gradient + term
    fresh = decay_rate * hessian[span, :] + gradient * gradient
    new_hessian[...] = fresh
    step[...] = jnp.clip(momentum[span, :] / (clip_scale * fresh), -1.0, 1.0)


def local(sizes, hidden, labels, weight, hessian, momentum):
    reps, shards, group = sizes
    vocab_rows = weight.shape[0]
    rows, columns = hidden.shape[0], hessian.shape[1]
    width = shards * rows

    hidden, own, parts, beside = begin_gather(hidden, sizes)
    mine = pl.pallas_call(
        label_kernel,
        in_specs=vmem_specs(1),
        out_specs=pl.BlockSpec(memory_space=pltpu.VMEM),
        out_shape=jax.ShapeDtypeStruct((1, width), jnp.float32),
        compiler_params=pltpu.CompilerParams(vmem_limit_bytes=MIB),
        name="label",
    )(after(labels[None], *own.values()))
    targets = [mine] + [xor_permute(mine, "rep", reps, j) for j in range(1, reps)]
    parts = [after(x, *own.values(), *targets) for x in parts]
    logits, kept, stats = [], [], []

    def consume(pieces):
        target = targets[len(logits)]
        block, found, columns_kept = logits_of(pieces, stats, target, weight, columns, rows)
        logits.append(weights_of(block, found, len(logits) * width))
        kept.append(columns_kept)
        stats.append(found)
        return found

    finish_gather(hidden, own, parts, beside, sizes, consume)
    stats = own_stats = stats[-1]
    for bits in (1 << b for b in range(group.bit_length() - 1)):
        other = xor_permute(stats, "tp", group, bits)
        stats = merge(False, MERGE_FLOPS, after(stats, *logits), other)
    others = [xor_permute(stats, "fsdp", shards, k) for k in range(1, shards)]
    stats = merge(True, 2 * MERGE_FLOPS, stats, *others)

    block = min(256, vocab_rows)
    tile = pl.BlockSpec((block, columns), lambda i: (i, 0))
    return pl.pallas_call(
        functools.partial(update_kernel, reps),
        grid=(vocab_rows // block,),
        in_specs=vmem_specs(2 * reps + 4),
        out_specs=[tile, tile],
        out_shape=[jax.ShapeDtypeStruct((vocab_rows, columns), jnp.float32)] * 2,
        compiler_params=pltpu.CompilerParams(vmem_limit_bytes=13 * MIB),
        cost_estimate=pl.CostEstimate(
            flops=0,
            bytes_accessed=16 * vocab_rows * columns,
            transcendentals=vocab_rows * width * reps,
        ),
        name="update",
    )(stats, own_stats, *logits, *kept, hessian, momentum)


def power_of_two(n):
    return n & (n - 1) == 0


def solution(mesh):
    placed = (
        P(("rep", "fsdp"), None),
        P(("rep", "fsdp")),
        P(("fsdp", "tp"), None),
        P(("fsdp", "tp"), "rep"),
        P(("fsdp", "tp"), "rep"),
    )
    sizes = tuple(mesh.shape[name] for name in ("rep", "fsdp", "tp"))

    def body(hidden, labels, weight, hessian, momentum):
        tokens = sizes[0] * sizes[1] * hidden.shape[0]
        fits = (
            all(power_of_two(n) for n in sizes)
            and sizes[1] > 2
            and sizes[2] > 2
            and sizes[0] * sizes[1] <= 8
            and hidden.shape[0] % 64 == 0
            and sizes[1] * hidden.shape[0] % LANE == 0
            and weight.shape[0] % 512 == 0
            and hessian.shape[1] % LANE == 0
            and tokens * hidden.shape[1] * 2 <= 4 * 1024 * 1024
            and 8 * hessian.size <= 32 * 1024 * 1024
        )
        if fits:
            return local(sizes, hidden, labels, weight, hessian, momentum)
        return local_large(hidden, labels, weight, hessian, momentum)

    return jax.shard_map(
        body,
        mesh=mesh,
        in_specs=placed,
        out_specs=(P(("fsdp", "tp"), "rep"), P(("fsdp", "tp"), "rep")),
        check_vma=False,
    )
```

```python
import functools
import math

import jax
import jax.numpy as jnp
from jax import lax
from jax.experimental import pallas as pl
from jax.experimental.pallas import tpu as pltpu
from jax.sharding import PartitionSpec as P

decay_rate = 0.99
clip_scale = 0.05


LANE = 128
MIB = 1024 * 1024
MERGE_FLOPS = 3 * 10**9
JOIN_FLOPS = 5 * 10**9


def local_large(hidden_states, labels, head_weight, hessian, momentum):
    vocab_rows = head_weight.shape[0]
    tokens, targets = (
        lax.all_gather(hidden_states, "fsdp", axis=0, tiled=True),
        lax.all_gather(labels, "fsdp", axis=0, tiled=True),
    )
    logits = lax.dot_general(
        tokens, head_weight, (((1,), (1,)), ((), ())), preferred_element_type=jnp.float32
    )
    local_max = jnp.max(logits, axis=1)
    row_max = lax.pmax(local_max, ("fsdp", "tp"))
    weights = jnp.exp(logits - row_max[:, None])
    row_total = lax.psum(jnp.sum(weights, axis=1), ("fsdp", "tp"))
    offset = lax.axis_index(("fsdp", "tp")) * vocab_rows
    columns = offset + lax.broadcasted_iota(jnp.int32, (1, vocab_rows), 1)
    onehot = (targets[:, None] == columns).astype(jnp.float32)
    residue = weights / row_total[:, None] - onehot
    partial_grad = lax.dot_general(
        residue,
        tokens.astype(jnp.float32),
        (((0,), (0,)), ((), ())),
        precision=lax.Precision.HIGHEST,
        preferred_element_type=jnp.float32,
    )
    gradient = lax.psum_scatter(partial_grad, "rep", scatter_dimension=1, tiled=True)
    new_hessian = decay_rate * hessian + (1.0 - decay_rate) * gradient * gradient
    step = jnp.clip(momentum / (clip_scale * new_hessian), -1.0, 1.0)
    return (new_hessian, step)


def xor_permute(x, axis, size, bits):
    return lax.ppermute(x, axis, [(i, i ^ bits) for i in range(size)])


def after(x, *others):
    return lax.optimization_barrier((x,) + others)[0]


def vmem_specs(n):
    return [pl.BlockSpec(memory_space=pltpu.VMEM)] * n


def position():
    member = lax.axis_index("tp")
    return lax.axis_index("fsdp"), lax.rem(member, 2), lax.rem(lax.div(member, 2), 2)


def cut_kernel(hidden, own, near, far):
    half, quarter = near.shape[0], far.shape[0]
    own[...] = hidden[...]
    _, side, part = position()
    near[...] = hidden[pl.ds(pl.multiple_of(side * half, half), half), :]
    first = pl.multiple_of(side * half + part * quarter, quarter)
    far[...] = hidden[pl.ds(first, quarter), :]


def label_kernel(labels, placed):
    shard, _, _ = position()
    values = labels[...].astype(jnp.float32)
    rows = values.shape[1]
    for k in range(placed.shape[1] // rows):
        placed[:, k * rows:(k + 1) * rows] = jnp.where(shard == k, values, 0.0)


def join_kernel(count, *refs):
    joined = refs[-1]
    at = 0
    for piece in refs[:count]:
        joined[at:at + piece.shape[0], :] = piece[...]
        at += piece.shape[0]


def begin_gather(hidden, sizes):
    reps, shards, _ = sizes
    rows, depth = hidden.shape
    kept, near, far = pl.pallas_call(
        cut_kernel,
        in_specs=vmem_specs(1),
        out_specs=vmem_specs(3),
        out_shape=[
            jax.ShapeDtypeStruct((rows, depth), hidden.dtype),
            jax.ShapeDtypeStruct((rows // 2, depth), hidden.dtype),
            jax.ShapeDtypeStruct((rows // 4, depth), hidden.dtype),
        ],
        compiler_params=pltpu.CompilerParams(vmem_limit_bytes=4 * MIB),
        name="cut",
    )(hidden)
    own = {j: xor_permute(near, "rep", reps, j) for j in range(1, reps)}
    parts = [xor_permute(far, "fsdp", shards, k) for k in range(2, shards)]
    beside = xor_permute(near, "fsdp", shards, 1)
    return kept, own, parts, beside


def finish_gather(hidden, own, parts, beside, sizes, consume):
    reps, shards, group = sizes
    distant = range(2, shards)
    joined = pl.pallas_call(
        functools.partial(join_kernel, len(parts)),
        in_specs=vmem_specs(len(parts)) + [],
        out_specs=pl.BlockSpec(memory_space=pltpu.VMEM),
        out_shape=jax.ShapeDtypeStruct(
            (len(parts) * parts[0].shape[0], hidden.shape[1]), hidden.dtype
        ),
        compiler_params=pltpu.CompilerParams(vmem_limit_bytes=4 * MIB),
        cost_estimate=pl.CostEstimate(flops=JOIN_FLOPS, bytes_accessed=0, transcendentals=0),
        name="join",
    )(*parts)

    def both_sides(x, segments):
        there = xor_permute(x, "tp", group, 1)
        other = [(k, 1, part) for k, _, part in segments]
        return [(x, segments), (there, other)]

    def members(pair, mixed, across):
        found = both_sides(pair, [(1, 0, None)])
        found += both_sides(mixed, [(k, 0, 0) for k in distant])
        return found + both_sides(across, [(k, 0, 1) for k in distant])

    theirs = {}
    for j in range(1, reps):
        mixed = xor_permute(joined, "rep", reps, j)
        pair = xor_permute(after(beside, mixed), "rep", reps, j)
        theirs[j] = both_sides(own[j], [(0, 0, None)]), pair, mixed
    across = xor_permute(joined, "tp", group, 2)
    token = consume([(hidden, [(0, None, None)])] + members(beside, joined, across))
    for j, (first, pair, mixed) in theirs.items():
        across = xor_permute(mixed, "tp", group, 2)
        token = consume(
            first + members(after(pair, token), mixed, after(across, token))
        )


def logits_kernel(segments, block_rows, column_axis, previous, weight, *refs):
    count = len(segments)
    pieces, earlier, target = refs[:count], refs[count:count + previous], refs[count + previous]
    logits, stats, kept, tokens = refs[count + previous + 1:]
    width, columns = tokens.shape[0], kept.shape[1]
    done = previous * width

    @pl.when(pl.program_id(0) == 0)
    def _():
        shard, side, part = position()
        for piece, places in zip(pieces, segments):
            size = piece.shape[0] // len(places)
            for i, (k, other_side, other_part) in enumerate(places):
                first = (shard ^ k) * block_rows
                if other_side is not None:
                    first += (side ^ other_side) * (block_rows // 2)
                if other_part is not None:
                    first += (part ^ other_part) * (block_rows // 4)
                first = pl.multiple_of(first, size)
                tokens[pl.ds(first, size), :] = piece[i * size:(i + 1) * size, :]
        first = pl.multiple_of(lax.axis_index(column_axis) * columns, LANE)
        kept[...] = tokens[:, pl.ds(first, columns)]
        for i, piece in enumerate(earlier):
            stats[:, i * width:(i + 1) * width] = piece[:, i * width:]
        stats[0:1, done:] = jnp.full((1, width), -jnp.inf, jnp.float32)
        stats[1:2, done:] = jnp.zeros((1, width), jnp.float32)
        stats[2:3, done:] = target[...]

    block = lax.dot_general(
        weight[...], tokens[...], (((1,), (1,)), ((), ())), preferred_element_type=jnp.float32
    )
    rows = block.shape[0]
    logits[pl.ds(pl.multiple_of(pl.program_id(0) * rows, rows), rows), :] = block
    before = stats[0:1, done:]
    now = jnp.maximum(before, jnp.max(block, axis=0, keepdims=True))
    stats[1:2, done:] = stats[1:2, done:] * jnp.exp(before - now) + jnp.sum(
        jnp.exp(block - now), axis=0, keepdims=True
    )
    stats[0:1, done:] = now


def logits_of(pieces, earlier, target, weight, columns, block_rows):
    vocab_rows, depth = weight.shape
    arrays = [x for x, _ in pieces]
    segments = tuple(tuple(places) for _, places in pieces)
    tokens = sum(x.shape[0] for x in arrays)
    block = min(512, vocab_rows)
    return pl.pallas_call(
        functools.partial(logits_kernel, segments, block_rows, "rep", len(earlier)),
        grid=(vocab_rows // block,),
        in_specs=[pl.BlockSpec((block, depth), lambda i: (i, 0))]
        + vmem_specs(len(arrays) + len(earlier) + 1),
        out_specs=vmem_specs(3),
        out_shape=[
            jax.ShapeDtypeStruct((vocab_rows, tokens), jnp.float32),
            jax.ShapeDtypeStruct((3, tokens * (1 + len(earlier))), jnp.float32),
            jax.ShapeDtypeStruct((tokens, columns), jnp.bfloat16),
        ],
        scratch_shapes=[pltpu.VMEM((tokens, depth), jnp.bfloat16)],
        compiler_params=pltpu.CompilerParams(vmem_limit_bytes=14 * MIB),
        cost_estimate=pl.CostEstimate(
            flops=2 * vocab_rows * depth * tokens,
            bytes_accessed=2 * vocab_rows * depth,
            transcendentals=vocab_rows * tokens,
        ),
        name="logits",
    )(weight, *arrays, *earlier, target)


def merge_kernel(labels_too, *refs):
    parts, merged = refs[:-1], refs[-1]
    top = parts[0][0:1, :]
    for part in parts[1:]:
        top = jnp.maximum(top, part[0:1, :])
    full, label = 0.0, parts[0][2:3, :]
    for part in parts:
        full += part[1:2, :] * jnp.exp(part[0:1, :] - top)
    if labels_too:
        for part in parts[1:]:
            label += part[2:3, :]
    merged[0:1, :], merged[1:2, :], merged[2:3, :] = top, full, label


def merge(labels_too, flops, *parts):
    stats = parts[0]
    return pl.pallas_call(
        functools.partial(merge_kernel, labels_too),
        in_specs=vmem_specs(len(parts)),
        out_specs=pl.BlockSpec(memory_space=pltpu.VMEM),
        out_shape=jax.ShapeDtypeStruct(stats.shape, stats.dtype),
        compiler_params=pltpu.CompilerParams(vmem_limit_bytes=MIB),
        cost_estimate=pl.CostEstimate(flops=flops, bytes_accessed=0, transcendentals=0),
        name="merge",
    )(*parts)


def weight_kernel(done, logits, stats, weights):
    width = logits.shape[1]
    weights[...] = jnp.exp(logits[...] - stats[0:1, done:done + width])


def weights_of(logits, stats, done):
    return pl.pallas_call(
        functools.partial(weight_kernel, done),
        in_specs=vmem_specs(2),
        out_specs=pl.BlockSpec(memory_space=pltpu.VMEM),
        out_shape=jax.ShapeDtypeStruct(logits.shape, logits.dtype),
        compiler_params=pltpu.CompilerParams(vmem_limit_bytes=2 * MIB),
        cost_estimate=pl.CostEstimate(flops=100000000, bytes_accessed=0, transcendentals=0),
        name="weights",
    )(logits, stats)


def update_kernel(groups, stats, own_stats, *refs):
    weights, tokens = refs[:groups], refs[groups:2 * groups]
    hessian, momentum, new_hessian, step = refs[2 * groups:]
    rows = new_hessian.shape[0]
    base = pl.multiple_of(pl.program_id(0) * rows, rows)
    span = pl.ds(base, rows)
    width = weights[0].shape[1]
    first = lax.axis_index(("fsdp", "tp")) * weights[0].shape[0] + base
    root = math.sqrt(1.0 - decay_rate)
    factor = root * jnp.exp(own_stats[0:1, :] - stats[0:1, :]) / stats[1:2, :]
    target = stats[2:3, :].astype(jnp.int32)
    gradient = None
    for j in range(groups):
        cols = slice(j * width, (j + 1) * width)
        block = weights[j][span, :]
        own = first + lax.broadcasted_iota(jnp.int32, block.shape, 0)
        onehot = jnp.where(own == target[:, cols], root, 0.0)
        residue = block * factor[:, cols] - onehot
        high = residue.astype(jnp.bfloat16)
        low = (residue - high.astype(jnp.float32)).astype(jnp.bfloat16)
        for term in (high, low):
            term = lax.dot_general(
                term, tokens[j][...], (((1,), (0,)), ((), ())), preferred_element_type=jnp.float32
            )
            gradient = term if gradient is None else gradient + term
    fresh = decay_rate * hessian[span, :] + gradient * gradient
    new_hessian[...] = fresh
    step[...] = jnp.clip(momentum[span, :] / (clip_scale * fresh), -1.0, 1.0)


def local(sizes, hidden, labels, weight, hessian, momentum):
    reps, shards, group = sizes
    vocab_rows = weight.shape[0]
    rows, columns = hidden.shape[0], hessian.shape[1]
    width = shards * rows

    hidden, own, parts, beside = begin_gather(hidden, sizes)
    mine = pl.pallas_call(
        label_kernel,
        in_specs=vmem_specs(1),
        out_specs=pl.BlockSpec(memory_space=pltpu.VMEM),
        out_shape=jax.ShapeDtypeStruct((1, width), jnp.float32),
        compiler_params=pltpu.CompilerParams(vmem_limit_bytes=MIB),
        name="label",
    )(after(labels[None], *own.values()))
    targets = [mine] + [xor_permute(mine, "rep", reps, j) for j in range(1, reps)]
    parts = [after(x, *own.values(), *targets) for x in parts]
    logits, kept, stats = [], [], []

    def consume(pieces):
        target = targets[len(logits)]
        block, found, columns_kept = logits_of(pieces, stats, target, weight, columns, rows)
        logits.append(weights_of(block, found, len(logits) * width))
        kept.append(columns_kept)
        stats.append(found)
        return found

    finish_gather(hidden, own, parts, beside, sizes, consume)
    stats = own_stats = stats[-1]
    others = [xor_permute(stats, "fsdp", shards, k) for k in range(1, shards)]
    stats = merge(True, 2 * MERGE_FLOPS, after(stats, *logits), *others)
    for bits in (1 << b for b in reversed(range(group.bit_length() - 1))):
        stats = merge(False, MERGE_FLOPS, stats, xor_permute(stats, "tp", group, bits))

    block = min(256, vocab_rows)
    tile = pl.BlockSpec((block, columns), lambda i: (i, 0))
    return pl.pallas_call(
        functools.partial(update_kernel, reps),
        grid=(vocab_rows // block,),
        in_specs=vmem_specs(2 * reps + 4),
        out_specs=[tile, tile],
        out_shape=[jax.ShapeDtypeStruct((vocab_rows, columns), jnp.float32)] * 2,
        compiler_params=pltpu.CompilerParams(vmem_limit_bytes=13 * MIB),
        cost_estimate=pl.CostEstimate(
            flops=0,
            bytes_accessed=16 * vocab_rows * columns,
            transcendentals=vocab_rows * width * reps,
        ),
        name="update",
    )(stats, own_stats, *logits, *kept, hessian, momentum)


def power_of_two(n):
    return n & (n - 1) == 0


def solution(mesh):
    placed = (
        P(("rep", "fsdp"), None),
        P(("rep", "fsdp")),
        P(("fsdp", "tp"), None),
        P(("fsdp", "tp"), "rep"),
        P(("fsdp", "tp"), "rep"),
    )
    sizes = tuple(mesh.shape[name] for name in ("rep", "fsdp", "tp"))

    def body(hidden, labels, weight, hessian, momentum):
        tokens = sizes[0] * sizes[1] * hidden.shape[0]
        fits = (
            all(power_of_two(n) for n in sizes)
            and sizes[1] > 2
            and sizes[2] > 2
            and sizes[0] * sizes[1] <= 8
            and hidden.shape[0] % 64 == 0
            and sizes[1] * hidden.shape[0] % LANE == 0
            and weight.shape[0] % 512 == 0
            and hessian.shape[1] % LANE == 0
            and tokens * hidden.shape[1] * 2 <= 4 * 1024 * 1024
            and 8 * hessian.size <= 32 * 1024 * 1024
        )
        if fits:
            return local(sizes, hidden, labels, weight, hessian, momentum)
        return local_large(hidden, labels, weight, hessian, momentum)

    return jax.shard_map(
        body,
        mesh=mesh,
        in_specs=placed,
        out_specs=(P(("fsdp", "tp"), "rep"), P(("fsdp", "tp"), "rep")),
        check_vma=False,
    )
```
